128 devices in a mesh: neg: 16 (over x, y), qry: 8 (over z, core).
Axes of the slice: x: 4, y: 4, z: 4, core: 2. Of those that a mesh axis runs over, the one named last changes fastest.
Arguments:
- items_table: bfloat16 [131072, 512], P('neg'), may hold values from -6 to 6
- fetch_rows: int32 [2048, 640], P(('neg', 'qry')), may hold values from 0 to 8191, as said below
- neighbour_slots: int32 [65536, 40], P(('neg', 'qry')), may hold values from 0 to 10239, as said below
- neighbour_count: int32 [65536], P(('neg', 'qry')), may hold values from 20 to 40
- self_slot: int32 [65536], P(('neg', 'qry')), may hold values from 0 to 10239
- negative_count: int32 [65536], P('neg'), may hold values from 1 to 999
- message_weight: bfloat16 [512, 512], replicated, may hold values from -0.25 to 0.25
- message_bias: float32 [512], replicated, may hold values from -3 to 3
- self_weight: bfloat16 [512, 512], replicated, may hold values from -0.25 to 0.25
- neighbour_weight: bfloat16 [512, 512], replicated, may hold values from -0.25 to 0.25
- output_bias: float32 [512], replicated, may hold values from -3 to 3
- queries: bfloat16 [8192, 512], P('qry'), may hold values from -8 to 8
Outputs:
- negative_embed: bfloat16 [65536, 512], P(('neg', 'qry'))
- query_lse: float32 [8192], P('qry')
The draws below stay inside these ranges and needn't reach their ends.
Inputs may be any that keep to these rules, and one draw needn't show every extreme that they name: Within one row of fetch_rows (one device's list for one partition) no item appears twice. `neighbour_slots`: every one of a device's 16 * 640 fetched rows is named by at least one live neighbour of that device's negatives.
All inputs are finite; a program needn't handle non-finite values.
Results may differ from the reference program's by a relative error of at most 0.0055.
Values may be sent and summed in bfloat16 or wider, within the bound.
No kernel may reach another device: no remote copies, remote signals or barrier semaphores. Data moves between devices by JAX's collectives and lax.ppermute only.
A program may use at most 128 MiB of HBM per device.

```python
import math
import jax
import jax.numpy as jnp
from jax import lax

D = 512
K = 40
ITEM_DEV = 8192
NEG_DEV = 512
CAP = 640
NEG = 65536
QRY = 8192
ITEMS = 131072
N_NEG = 16
N_QRY = 8


def draw_queries(key, part):
    values = jnp.clip(jax.random.normal(key, (QRY, D), jnp.float32), -5.5, 5.5)
    return values.astype(jnp.bfloat16)


def draw_fetch_rows(key, part):
    row_keys = jax.random.split(jax.random.fold_in(key, 7), N_NEG * N_QRY * N_NEG)

    def one_row(row_key):
        return jax.random.permutation(row_key, ITEM_DEV)[:CAP].astype(jnp.int32)
    return jax.vmap(one_row)(row_keys).astype(jnp.int32)


def neighbour_draw(key):
    count_key = jax.random.fold_in(key, 11)
    counts = jax.random.randint(count_key, (NEG,), K // 2, K + 1, dtype=jnp.int32)
    slot_total = N_NEG * CAP
    device_keys = jax.random.split(jax.random.fold_in(key, 13), N_NEG * N_QRY)
    count_blocks = counts.reshape(N_NEG * N_QRY, NEG_DEV)

    def one_device(device_key, count_block):
        order_key = jax.random.fold_in(device_key, 1)
        filler_key = jax.random.fold_in(device_key, 2)
        live_mask = jnp.arange(K, dtype=jnp.int32)[None, :] < count_block[:, None]
        priority = jax.random.randint(order_key, (NEG_DEV * K,), 0, 1 << 20, dtype=jnp.int32)
        priority = priority + jnp.where(live_mask.reshape(-1), 0, 1 << 21).astype(jnp.int32)
        order = jnp.argsort(priority, stable=True).astype(jnp.int32)
        ranked = jnp.argsort(order, stable=True).astype(jnp.int32)
        filler = jax.random.randint(filler_key, (NEG_DEV * K,), 0, slot_total, dtype=jnp.int32)
        slots = jnp.where(ranked < slot_total, ranked, filler)
        return slots.reshape(NEG_DEV, K).astype(jnp.int32)
    slots = jax.vmap(one_device)(device_keys, count_blocks).reshape(NEG, K)
    return (counts, slots)


def draw_neighbour_count(key, part):
    return neighbour_draw(key)[0].astype(jnp.int32)


def draw_neighbour_slots(key, part):
    return neighbour_draw(key)[1].astype(jnp.int32)


def place_ends(drawn, stream_key, smallest, largest):
    longest = drawn.shape.index(max(drawn.shape))
    spots = []
    for shift in (0, 1):
        where = [jax.random.randint(jax.random.fold_in(stream_key, axis), (), 0, length) for axis, length in enumerate(drawn.shape)]
        where[longest] = (where[longest] + shift) % drawn.shape[longest]
        spots.append(tuple(where))
    return drawn.at[spots[0]].set(smallest).at[spots[1]].set(largest)


def shard_levels(own_key, shape, cuts, least, high):
    factor_of = 1.0
    for dim, parts in cuts:
        draws = jax.random.uniform(jax.random.fold_in(jax.random.fold_in(own_key, 6), dim), (parts,), jnp.float32, least / len(cuts), high / len(cuts))
        factor_of = factor_of * jnp.repeat(jnp.exp(draws), shape[dim] // parts).reshape((-1,) + (1,) * (len(shape) - 1 - dim))
    return factor_of


def gaussian(key, shape, deviation, limit, pieces=(), kind=jnp.bfloat16):
    factor_of = shard_levels(key, shape, pieces, -0.22, 0.18) if pieces else 1.0
    values = jax.random.normal(key, shape, jnp.float32) * deviation * factor_of
    return jnp.minimum(jnp.maximum(values, -limit), limit).astype(kind)


def setup_inputs(seed: int = 0) -> dict:
    seeds = jax.random.split(jax.random.key(seed), 13)
    items_table = gaussian(seeds[0], (ITEMS, D), 1.0, 6.0, ((0, 16),))
    fetch_rows = draw_fetch_rows(jax.random.fold_in(seeds[12], 71), 0)
    neighbour_slots = draw_neighbour_slots(jax.random.fold_in(seeds[12], 71), 0)
    neighbour_count = draw_neighbour_count(jax.random.fold_in(seeds[12], 71), 0)
    self_slot = place_ends(jax.random.randint(seeds[4], (NEG,), 0, N_NEG * CAP), jax.random.fold_in(seeds[4], 1), 0, (N_NEG * CAP) - 1).astype(jnp.int32)
    negative_count = place_ends(jax.random.randint(seeds[5], (NEG,), 1, 1000), jax.random.fold_in(seeds[5], 1), 1, 999).astype(jnp.int32)
    message_weight = gaussian(seeds[6], (D, D), D ** -0.5, 0.25)
    message_bias = gaussian(seeds[7], (D,), 0.5, 3.0, (), jnp.float32)
    self_weight = gaussian(seeds[8], (D, D), D ** -0.5, 0.25)
    neighbour_weight = gaussian(seeds[9], (D, D), D ** -0.5, 0.25)
    output_bias = gaussian(seeds[10], (D,), 0.5, 3.0, (), jnp.float32)
    queries = draw_queries(jax.random.fold_in(seeds[12], 71), 0)
    return {"items_table": items_table, "fetch_rows": fetch_rows, "neighbour_slots": neighbour_slots, "neighbour_count": neighbour_count, "self_slot": self_slot, "negative_count": negative_count, "message_weight": message_weight, "message_bias": message_bias, "self_weight": self_weight, "neighbour_weight": neighbour_weight, "output_bias": output_bias, "queries": queries}


def embed_device(items_table, fetch_block, slot_block, count_block, self_block, message_weight, message_bias, self_weight, neighbour_weight, output_bias):
    owners = jnp.arange(N_NEG, dtype=jnp.int32)[:, None] * ITEM_DEV
    global_rows = (fetch_block.astype(jnp.int32) + owners).reshape(-1)
    fetched = items_table[global_rows]
    message = jax.nn.relu(jnp.dot(fetched, message_weight, preferred_element_type=jnp.float32) + message_bias).astype(jnp.bfloat16)
    gathered = message[slot_block].astype(jnp.float32)
    live_mask = jnp.arange(K, dtype=jnp.int32)[None, :] < count_block[:, None]
    summed = lax.optimization_barrier(jnp.sum(jnp.where(live_mask[:, :, None], gathered, jnp.float32(0.0)), axis=1))
    neighbour_mean = (summed / count_block.astype(jnp.float32)[:, None]).astype(jnp.bfloat16)
    self_rows = fetched[self_block]
    hidden = jnp.dot(self_rows, self_weight, preferred_element_type=jnp.float32)
    hidden = hidden + jnp.dot(neighbour_mean, neighbour_weight, preferred_element_type=jnp.float32) + output_bias
    hidden = jax.nn.relu(hidden)
    scale_inv = lax.rsqrt(lax.optimization_barrier(jnp.mean(hidden * hidden, axis=-1, keepdims=True)) + 0.25)
    return (hidden * scale_inv).astype(jnp.bfloat16)

def reference(items_table, fetch_rows, neighbour_slots, neighbour_count, self_slot, negative_count, message_weight, message_bias, self_weight, neighbour_weight, output_bias, queries):
    devices_all = N_NEG * N_QRY
    fetch_all = fetch_rows.reshape(devices_all, N_NEG, -1)
    slots_all = neighbour_slots.reshape(devices_all, -1, K)
    counts_all = neighbour_count.reshape(devices_all, -1)
    selves_all = self_slot.reshape(devices_all, -1)

    def one_device(inputs):
        return embed_device(items_table, inputs[0], inputs[1], inputs[2], inputs[3], message_weight, message_bias, self_weight, neighbour_weight, output_bias)
    embedded = lax.map(one_device, (fetch_all, slots_all, counts_all, selves_all))
    negative_embed = embedded.reshape(-1, D)
    log_count = jnp.log(negative_count.astype(jnp.float32))
    query_blocks = queries.reshape(N_QRY, -1, D)

    def one_block(query_block):
        scores = 0.25 * jnp.dot(query_block, negative_embed.T, preferred_element_type=jnp.float32) - log_count[None, :]
        peak = lax.optimization_barrier(jnp.max(scores, axis=1))
        totals = lax.optimization_barrier(jnp.sum(jnp.exp(scores - peak[:, None]), axis=1))
        return peak + jnp.log(totals) - math.log(NEG)
    query_lse = lax.map(one_block, query_blocks).reshape(-1)
    return (negative_embed, query_lse)
```

```python
import functools
import math

import jax
import jax.numpy as jnp
from jax import lax
from jax.experimental import pallas as pl
from jax.experimental.pallas import tpu as pltpu
from jax.sharding import PartitionSpec as P

LANES = 128
DEAD = 2**31 - 1
CHUNK = 128
STRIDE = 132
BLOCK = 10
STAGE = 1024


def compose_kernel(slots_ref, self_ref, count_ref, fetch_ref, keys_ref):
    neighbours = slots_ref.shape[0]
    columns = slots_ref.shape[1] // LANES
    rows = fetch_ref.shape[0]
    count = count_ref[...]

    def looked_up(slots):
        hi = [s >> 7 for s in slots]
        lo = [s & 127 for s in slots]

        def step(h, found):
            line = jnp.broadcast_to(fetch_ref[pl.ds(h, 1), :], (8, LANES))
            return tuple(
                jnp.where(hi[i] == h, jnp.take_along_axis(line, lo[i], axis=1), found[i])
                for i in range(len(slots))
            )

        found = lax.fori_loop(0, rows, step, tuple(jnp.zeros_like(s) for s in slots))
        return hi, found

    def key_of(hi, row, v):
        part = (hi * 205) >> 10
        return ((part - 8) << 28) | (v << 19) | row

    for j in range(columns):
        lane = slice(j * LANES, (j + 1) * LANES)
        v = lax.broadcasted_iota(jnp.int32, (8, LANES), 1) + j * LANES
        cnt = jnp.broadcast_to(count[:, lane], (8, LANES))
        slots = [slots_ref[8 * i : 8 * (i + 1), lane] for i in range(neighbours // 8)]
        slots.append(jnp.broadcast_to(self_ref[:, lane], (8, LANES)))
        hi, found = looked_up(slots)
        for i in range(neighbours // 8):
            k = lax.broadcasted_iota(jnp.int32, (8, LANES), 0) + 8 * i
            key = key_of(hi[i], found[i], v)
            keys_ref[8 * i : 8 * (i + 1), lane] = jnp.where(k < cnt, key, DEAD)
        own = key_of(hi[-1], found[-1], v) | ((cnt - 20) << 14) | (1 << 13)
        keys_ref[neighbours : neighbours + 1, lane] = own[:1]


def owner_kernel(
    part_ref, list_smem, list_vmem, message_hbm, self_hbm, out_ref,
    table, stage, pick, rows, acc, sems,
):
    entries = 164
    items = message_hbm.shape[0]
    width = message_hbm.shape[1]
    tiles = width // LANES
    per_table = items // STAGE

    def stage_copy(c):
        source = message_hbm if c < per_table else self_hbm
        return pltpu.make_async_copy(
            source.at[pl.ds((c % per_table) * STAGE, STAGE), :], stage.at[c % 2], sems.at[c % 2]
        )

    @pl.when(pl.program_id(0) == 0)
    def _():
        stage_copy(0).start()
        rows[...] = jnp.zeros_like(rows)
        for c in range(2 * per_table):
            if c + 1 < 2 * per_table:
                stage_copy(c + 1).start()
            stage_copy(c).wait()

            def spread(i, _, c=c):
                for u in range(4):
                    at = pl.multiple_of(i * 64 + u * 16, 16)
                    block = stage[c % 2, pl.ds(at, 16), :].astype(jnp.float32)
                    for half in range(2):
                        for j in range(tiles):
                            first = (c * STAGE + at + half * 8) * tiles + j
                            table[pl.ds(first, 8, stride=tiles), :] = block[
                                half * 8 : half * 8 + 8, j * LANES : (j + 1) * LANES
                            ]
                return 0

            lax.fori_loop(0, STAGE // 64, spread, 0)

    part = part_ref[0]
    end = list_smem[0, entries, part]
    start = jnp.where(part == 0, 0, list_smem[0, entries, jnp.maximum(part - 1, 0)])
    row_first = start >> 7
    row_last = (end + 127) >> 7
    negatives = out_ref.shape[0]

    def one_block(base):
        for c in range(BLOCK):
            r = base + c

            @pl.when(r < row_last)
            def _(c=c, r=r):
                line = list_vmem[0, pl.ds(r, 1), :]
                at = r * LANES + lax.broadcasted_iota(jnp.int32, (1, LANES), 1)
                live = (at >= start) & (at < end)
                who = jnp.where(live, (line >> 19) & 511, -1)
                weight = jnp.where((line & 8192) != 0, ((line >> 14) & 31) + 20, 1).astype(jnp.float32)
                v = lax.broadcasted_iota(jnp.int32, (negatives, LANES), 0)
                pick[:, c * LANES : (c + 1) * LANES] = jnp.where(v == who, weight, 0.0).astype(jnp.bfloat16)
                for e in range(CHUNK):
                    t = list_smem[0, r, e] & 16383
                    slab = table[pl.ds(pl.multiple_of(t * tiles, tiles), tiles), :]
                    rows[c, pl.ds(e, tiles, stride=STRIDE), :] = slab

            @pl.when(r >= row_last)
            def _(c=c):
                pick[:, c * LANES : (c + 1) * LANES] = jnp.zeros((negatives, LANES), jnp.bfloat16)

        gathered = jnp.concatenate(
            [
                jnp.concatenate(
                    [rows[c, j * STRIDE : j * STRIDE + CHUNK, :].astype(jnp.bfloat16) for j in range(tiles)],
                    axis=1,
                )
                for c in range(BLOCK)
            ],
            axis=0,
        )
        return jnp.dot(pick[...], gathered, preferred_element_type=jnp.float32)

    acc[...] = one_block(row_first)

    def more(i, _):
        acc[...] += one_block(row_first + i * BLOCK)
        return 0

    lax.fori_loop(1, (row_last - row_first + BLOCK - 1) // BLOCK, more, 0)
    out_ref[...] = acc[...].astype(jnp.bfloat16)


def from_everyone(x, axis):
    devices = lax.axis_size(axis)
    return lax.all_to_all(jnp.broadcast_to(x[None], (devices, *x.shape)), axis, 0, 0, tiled=True)


def composed_keys(neighbour_slots, self_slot, neighbour_count, fetch_rows):
    negatives, neighbours = neighbour_slots.shape
    return pl.pallas_call(
        compose_kernel,
        out_shape=jax.ShapeDtypeStruct((neighbours + 1, negatives), jnp.int32),
        name="compose",
    )(
        neighbour_slots.T,
        self_slot[None, :],
        neighbour_count[None, :],
        fetch_rows.reshape(-1, LANES),
    )


def owner_sums(part, lists, message_part, self_part, negatives):
    devices, lines, _ = lists.shape
    items, width = message_part.shape
    tiles = width // LANES
    return pl.pallas_call(
        owner_kernel,
        grid=(devices,),
        in_specs=[
            pl.BlockSpec(memory_space=pltpu.SMEM),
            pl.BlockSpec((1, lines, LANES), lambda a: (a, 0, 0), memory_space=pltpu.SMEM),
            pl.BlockSpec((1, lines, LANES), lambda a: (a, 0, 0)),
            pl.BlockSpec(memory_space=pl.ANY),
            pl.BlockSpec(memory_space=pl.ANY),
        ],
        out_specs=pl.BlockSpec((negatives, width), lambda a: (a, 0)),
        out_shape=jax.ShapeDtypeStruct((devices * negatives, width), jnp.bfloat16),
        scratch_shapes=[
            pltpu.VMEM((2 * items * tiles, LANES), jnp.float32),
            pltpu.VMEM((2, STAGE, width), jnp.bfloat16),
            pltpu.VMEM((negatives, BLOCK * CHUNK), jnp.bfloat16),
            pltpu.VMEM((BLOCK, tiles * STRIDE, LANES), jnp.float32),
            pltpu.VMEM((negatives, width), jnp.float32),
            pltpu.SemaphoreType.DMA((2,)),
        ],
        compiler_params=pltpu.CompilerParams(
            dimension_semantics=("arbitrary",), vmem_limit_bytes=60 * 2**20
        ),
        name="owner",
    )(part, lists, lists, message_part, self_part)


def per_device(
    items_table,
    fetch_rows,
    neighbour_slots,
    neighbour_count,
    self_slot,
    negative_count,
    message_weight,
    message_bias,
    self_weight,
    neighbour_weight,
    output_bias,
    queries,
):
    f32 = jnp.float32
    negatives = neighbour_count.shape[0]
    parts = lax.axis_size("neg")
    groups = lax.axis_size("qry")
    queries_all = lax.all_gather(queries, "qry", axis=0, tiled=True)

    keys = composed_keys(neighbour_slots, self_slot, neighbour_count, fetch_rows).reshape(-1)
    bounds = jnp.array([min((p + 1 - 8) << 28, DEAD) for p in range(parts)], jnp.int32)
    ends = jnp.sum((keys[None, :] < bounds[:, None]).astype(jnp.int32), axis=1)
    lines = jnp.concatenate([lax.sort(keys, is_stable=False), ends, jnp.zeros((184 * LANES - keys.size - parts,), jnp.int32)])
    lists = from_everyone(lines.reshape(184, LANES), "neg")

    message = jax.nn.relu(
        jnp.dot(items_table, message_weight, preferred_element_type=f32) + message_bias
    ).astype(jnp.bfloat16)
    message_part = jnp.dot(message, neighbour_weight, preferred_element_type=f32).astype(jnp.bfloat16)
    self_part = jnp.dot(items_table, self_weight, preferred_element_type=f32).astype(jnp.bfloat16)

    partial = owner_sums(lax.axis_index("neg").reshape(1).astype(jnp.int32), lists, message_part, self_part, negatives)
    total = lax.psum_scatter(partial, "neg", scatter_dimension=0, tiled=True).astype(f32)

    hidden = jax.nn.relu(total / neighbour_count.astype(f32)[:, None] + output_bias)
    scale_inv = lax.rsqrt(jnp.mean(hidden * hidden, axis=-1, keepdims=True) + 0.25)
    negative_embed = (hidden * scale_inv).astype(jnp.bfloat16)

    own_count = lax.dynamic_slice(negative_count, (lax.axis_index("qry") * negatives,), (negatives,))
    log_count = jnp.log(own_count.astype(f32))
    scores = (
        0.25
        * lax.dot_general(negative_embed, queries_all, (((1,), (1,)), ((), ())), preferred_element_type=f32)
        - log_count[:, None]
    )
    peak = jnp.max(scores, axis=0)
    part_lse = peak + jnp.log(jnp.sum(jnp.exp(scores - peak[None, :]), axis=0))
    shared = jnp.broadcast_to(part_lse.reshape(1, groups, -1), (parts, groups, queries.shape[0]))
    parts_lse = lax.all_to_all(
        shared.reshape(parts * groups, -1), ("neg", "qry"), split_axis=0, concat_axis=0, tiled=True
    )
    top = jnp.max(parts_lse, axis=0)
    query_lse = top + jnp.log(jnp.sum(jnp.exp(parts_lse - top[None, :]), axis=0))
    return (negative_embed, query_lse - math.log(negatives * parts * groups))


def solution(mesh):
    in_specs = (
        P("neg", None),
        P(("neg", "qry"), None),
        P(("neg", "qry"), None),
        P(("neg", "qry")),
        P(("neg", "qry")),
        P("neg"),
        P(),
        P(),
        P(),
        P(),
        P(),
        P("qry", None),
    )
    out_specs = (P(("neg", "qry"), None), P("qry"))
    return jax.shard_map(
        per_device, mesh=mesh, in_specs=in_specs, out_specs=out_specs, check_vma=False
    )
```

```python
import functools
import math

import jax
import jax.numpy as jnp
from jax import lax
from jax.experimental import pallas as pl
from jax.experimental.pallas import tpu as pltpu
from jax.sharding import PartitionSpec as P

LANES = 128
DEAD = 2**31 - 1
CHUNK = 128
STRIDE = 132
BLOCK = 10
STAGE = 1024


def compose_kernel(slots_ref, self_ref, count_ref, own_count_ref, fetch_ref, keys_ref):
    neighbours, negatives = slots_ref.shape
    parts, per_part = fetch_ref.shape
    per_line = per_part // LANES
    half = parts // 2
    packed = fetch_ref[:half, :] | (fetch_ref[half:, :] << 13)
    lines = [
        jnp.broadcast_to(packed[p : p + 1, j * LANES : (j + 1) * LANES], (8, LANES))
        for p in range(half)
        for j in range(per_line)
    ]

    def located(slot):
        hi = slot >> 7
        lo = slot & 127
        upper = hi >= len(lines)
        folded = jnp.where(upper, hi - len(lines), hi)
        found = jnp.zeros_like(slot)
        for h, line in enumerate(lines):
            at = jnp.take_along_axis(line, lo, axis=1, mode="promise_in_bounds")
            found = jnp.where(folded == h, at, found)
        row = jnp.where(upper, found >> 13, found & 8191)
        return ((((hi * 205) >> 10) - 8) << 28) | row

    sublane = lax.broadcasted_iota(jnp.int32, (8, LANES), 0)
    lane = lax.broadcasted_iota(jnp.int32, (8, LANES), 1)
    for j in range(negatives // LANES):
        cols = slice(j * LANES, (j + 1) * LANES)
        count = jnp.broadcast_to(count_ref[:, cols], (8, LANES))
        for i in range(neighbours // 8):
            key = located(slots_ref[8 * i : 8 * (i + 1), cols]) | ((lane + j * LANES) << 19)
            first = (j * (neighbours // 8) + i) * 8
            keys_ref[first : first + 8, :] = jnp.where(sublane + 8 * i < count, key, DEAD)
    own = located(self_ref[...]) | ((sublane * LANES + lane) << 19)
    own = own | ((own_count_ref[...] - 20) << 14) | (1 << 13)
    keys_ref[neighbours * negatives // LANES :, :] = own[: negatives // LANES]


def owner_kernel(
    part_ref, ends_ref, lists_ref, message_hbm, self_hbm, out_ref,
    table, stage, pick, rows, acc, offsets, places, sems, place_sems,
):
    items = message_hbm.shape[0]
    width = message_hbm.shape[1]
    tiles = width // LANES
    per_table = items // STAGE
    a = pl.program_id(0)
    devices = pl.num_programs(0)
    part = part_ref[0]
    negatives = out_ref.shape[0]

    def range_of(r):
        return jnp.where(part == 0, 0, ends_ref[r, jnp.maximum(part - 1, 0)]), ends_ref[r, part]

    def place_copy(slot):
        return pltpu.make_async_copy(offsets.at[slot], places.at[slot], place_sems.at[slot])

    def place(r, base, slot):
        for c in range(BLOCK):
            line = lists_ref[r, pl.ds(base + c, 1), :]
            offsets[slot, c : c + 1, :] = (line & 16383) * tiles
        place_copy(slot).start()

    def stage_copy(c):
        source = message_hbm if c < per_table else self_hbm
        return pltpu.make_async_copy(
            source.at[pl.ds((c % per_table) * STAGE, STAGE), :], stage.at[c % 2], sems.at[c % 2]
        )

    @pl.when(a == 0)
    def _():
        stage_copy(0).start()
        place(0, range_of(0)[0] >> 7, 0)
        rows[...] = jnp.zeros_like(rows)
        for c in range(2 * per_table):
            if c + 1 < 2 * per_table:
                stage_copy(c + 1).start()
            stage_copy(c).wait()

            def spread(i, _, c=c):
                for u in range(4):
                    at = pl.multiple_of(i * 64 + u * 16, 16)
                    block = stage[c % 2, pl.ds(at, 16), :].astype(jnp.float32)
                    for half in range(2):
                        for j in range(tiles):
                            first = (c * STAGE + at + half * 8) * tiles + j
                            table[pl.ds(first, 8, stride=tiles), :] = block[
                                half * 8 : half * 8 + 8, j * LANES : (j + 1) * LANES
                            ]
                return 0

            lax.fori_loop(0, STAGE // 64, spread, 0)

    start, end = range_of(a)
    row_first = start >> 7
    row_last = (end + 127) >> 7

    def one_block(base, slot):
        place_copy(slot).wait()
        v = lax.broadcasted_iota(jnp.int32, (negatives, LANES), 0)
        lane = lax.broadcasted_iota(jnp.int32, (1, LANES), 1)
        for c in range(BLOCK):
            r = base + c

            @pl.when(r < row_last)
            def _(c=c, r=r):
                line = lists_ref[a, pl.ds(r, 1), :]
                at = r * LANES + lane
                who = jnp.where((at >= start) & (at < end), (line >> 19) & 511, -1)
                weight = jnp.where((line & 8192) != 0, ((line >> 14) & 31) + 20, 1).astype(jnp.float32)
                pick[:, c * LANES : (c + 1) * LANES] = jnp.where(v == who, weight, 0.0).astype(jnp.bfloat16)
                for e in range(CHUNK):
                    at = pl.multiple_of(places[slot, c, e], tiles)
                    rows[c, pl.ds(e, tiles, stride=STRIDE), :] = table[pl.ds(at, tiles), :]

            @pl.when(r >= row_last)
            def _(c=c):
                pick[:, c * LANES : (c + 1) * LANES] = jnp.zeros((negatives, LANES), jnp.bfloat16)

        gathered = jnp.concatenate(
            [
                jnp.concatenate(
                    [rows[c, j * STRIDE : j * STRIDE + CHUNK, :].astype(jnp.bfloat16) for j in range(tiles)],
                    axis=1,
                )
                for c in range(BLOCK)
            ],
            axis=0,
        )
        return jnp.dot(pick[...], gathered, preferred_element_type=jnp.float32)

    slot = a % 2

    @pl.when(a + 1 < devices)
    def _():
        place(a + 1, range_of(a + 1)[0] >> 7, 1 - slot)

    acc[...] = one_block(row_first, slot)

    def more(i, _):
        place(a, row_first + i * BLOCK, slot)
        acc[...] += one_block(row_first + i * BLOCK, slot)
        return 0

    lax.fori_loop(1, (row_last - row_first + BLOCK - 1) // BLOCK, more, 0)
    out_ref[...] = acc[...].astype(jnp.bfloat16)


def from_everyone(x, axis):
    devices = lax.axis_size(axis)
    return lax.all_to_all(jnp.broadcast_to(x[None], (devices, *x.shape)), axis, 0, 0, tiled=True)


def composed_keys(neighbour_slots, self_slot, neighbour_count, fetch_rows):
    negatives, neighbours = neighbour_slots.shape
    folded = negatives // LANES

    def tile_of(x):
        return jnp.pad(x.reshape(folded, LANES), ((0, 8 - folded), (0, 0)))

    return pl.pallas_call(
        compose_kernel,
        out_shape=jax.ShapeDtypeStruct(((neighbours + 1) * folded, LANES), jnp.int32),
        name="compose",
    )(
        neighbour_slots.T,
        tile_of(self_slot),
        neighbour_count[None, :],
        tile_of(neighbour_count),
        fetch_rows,
    )


def owner_sums(part, ends, lists, message_part, self_part, negatives):
    devices, lines, _ = lists.shape
    items, width = message_part.shape
    tiles = width // LANES
    return pl.pallas_call(
        owner_kernel,
        grid=(devices,),
        in_specs=[
            pl.BlockSpec(memory_space=pltpu.SMEM),
            pl.BlockSpec(memory_space=pltpu.SMEM),
            pl.BlockSpec(memory_space=pltpu.VMEM),
            pl.BlockSpec(memory_space=pl.ANY),
            pl.BlockSpec(memory_space=pl.ANY),
        ],
        out_specs=pl.BlockSpec((negatives, width), lambda a: (a, 0)),
        out_shape=jax.ShapeDtypeStruct((devices * negatives, width), jnp.bfloat16),
        scratch_shapes=[
            pltpu.VMEM((2 * items * tiles, LANES), jnp.float32),
            pltpu.VMEM((2, STAGE, width), jnp.bfloat16),
            pltpu.VMEM((negatives, BLOCK * CHUNK), jnp.bfloat16),
            pltpu.VMEM((BLOCK, tiles * STRIDE, LANES), jnp.float32),
            pltpu.VMEM((negatives, width), jnp.float32),
            pltpu.VMEM((2, 16, LANES), jnp.int32),
            pltpu.SMEM((2, 16, LANES), jnp.int32),
            pltpu.SemaphoreType.DMA((2,)),
            pltpu.SemaphoreType.DMA((2,)),
        ],
        compiler_params=pltpu.CompilerParams(
            dimension_semantics=("arbitrary",), vmem_limit_bytes=60 * 2**20
        ),
        name="owner",
    )(part, ends, lists, message_part, self_part)


def per_device(
    items_table,
    fetch_rows,
    neighbour_slots,
    neighbour_count,
    self_slot,
    negative_count,
    message_weight,
    message_bias,
    self_weight,
    neighbour_weight,
    output_bias,
    queries,
):
    f32 = jnp.float32
    negatives = neighbour_count.shape[0]
    parts = lax.axis_size("neg")
    groups = lax.axis_size("qry")
    queries_all = lax.all_gather(queries, "qry", axis=0, tiled=True)

    keys = composed_keys(neighbour_slots, self_slot, neighbour_count, fetch_rows).reshape(-1)
    bounds = jnp.array([min((p + 1 - 8) << 28, DEAD) for p in range(parts)], jnp.int32)
    ends = jnp.sum((keys[None, :] < bounds[:, None]).astype(jnp.int32), axis=1)
    lines = jnp.concatenate([lax.sort(keys, is_stable=False), ends, jnp.zeros((184 * LANES - keys.size - parts,), jnp.int32)])
    lists = from_everyone(lines.reshape(184, LANES), "neg")

    message = jax.nn.relu(
        jnp.dot(items_table, message_weight, preferred_element_type=f32) + message_bias
    ).astype(jnp.bfloat16)
    message_part = jnp.dot(message, neighbour_weight, preferred_element_type=f32).astype(jnp.bfloat16)
    self_part = jnp.dot(items_table, self_weight, preferred_element_type=f32).astype(jnp.bfloat16)

    part = lax.axis_index("neg").reshape(1).astype(jnp.int32)
    partial = owner_sums(part, lists[:, keys.size // LANES, :parts], lists, message_part, self_part, negatives)
    total = lax.psum_scatter(partial, "neg", scatter_dimension=0, tiled=True).astype(f32)

    hidden = jax.nn.relu(total / neighbour_count.astype(f32)[:, None] + output_bias)
    scale_inv = lax.rsqrt(jnp.mean(hidden * hidden, axis=-1, keepdims=True) + 0.25)
    negative_embed = (hidden * scale_inv).astype(jnp.bfloat16)

    own_count = lax.dynamic_slice(negative_count, (lax.axis_index("qry") * negatives,), (negatives,))
    log_count = jnp.log(own_count.astype(f32))
    scores = (
        0.25
        * lax.dot_general(negative_embed, queries_all, (((1,), (1,)), ((), ())), preferred_element_type=f32)
        - log_count[:, None]
    )
    peak = jnp.max(scores, axis=0)
    part_lse = peak + jnp.log(jnp.sum(jnp.exp(scores - peak[None, :]), axis=0))
    shared = jnp.broadcast_to(part_lse.reshape(1, groups, -1), (parts, groups, queries.shape[0]))
    parts_lse = lax.all_to_all(
        shared.reshape(parts * groups, -1), ("neg", "qry"), split_axis=0, concat_axis=0, tiled=True
    )
    top = jnp.max(parts_lse, axis=0)
    query_lse = top + jnp.log(jnp.sum(jnp.exp(parts_lse - top[None, :]), axis=0))
    return (negative_embed, query_lse - math.log(negatives * parts * groups))


def solution(mesh):
    in_specs = (
        P("neg", None),
        P(("neg", "qry"), None),
        P(("neg", "qry"), None),
        P(("neg", "qry")),
        P(("neg", "qry")),
        P("neg"),
        P(),
        P(),
        P(),
        P(),
        P(),
        P("qry", None),
    )
    out_specs = (P(("neg", "qry"), None), P("qry"))
    return jax.shard_map(
        per_device, mesh=mesh, in_specs=in_specs, out_specs=out_specs, check_vma=False
    )
```

```python
import functools
import math

import jax
import jax.numpy as jnp
from jax import lax
from jax.experimental import pallas as pl
from jax.experimental.pallas import tpu as pltpu
from jax.sharding import PartitionSpec as P

LANES = 128
DEAD = 2**31 - 1
CHUNK = 128
STRIDE = 132
BLOCK = 10
STAGE = 1024
SIDE = 4


def compose_kernel(slots_ref, self_ref, count_ref, own_count_ref, fetch_ref, keys_ref):
    neighbours, negatives = slots_ref.shape
    parts, per_part = fetch_ref.shape
    per_line = per_part // LANES
    half = parts // 2
    packed = fetch_ref[:half, :] | (fetch_ref[half:, :] << 13)
    lines = [
        jnp.broadcast_to(packed[p : p + 1, j * LANES : (j + 1) * LANES], (8, LANES))
        for p in range(half)
        for j in range(per_line)
    ]

    def located(slot):
        hi = slot >> 7
        lo = slot & 127
        upper = hi >= len(lines)
        folded = jnp.where(upper, hi - len(lines), hi)
        found = jnp.zeros_like(slot)
        for h, line in enumerate(lines):
            at = jnp.take_along_axis(line, lo, axis=1, mode="promise_in_bounds")
            found = jnp.where(folded == h, at, found)
        row = jnp.where(upper, found >> 13, found & 8191)
        return ((((hi * 205) >> 10) - 8) << 28) | row

    sublane = lax.broadcasted_iota(jnp.int32, (8, LANES), 0)
    lane = lax.broadcasted_iota(jnp.int32, (8, LANES), 1)
    for j in range(negatives // LANES):
        cols = slice(j * LANES, (j + 1) * LANES)
        count = jnp.broadcast_to(count_ref[:, cols], (8, LANES))
        for i in range(neighbours // 8):
            key = located(slots_ref[8 * i : 8 * (i + 1), cols]) | ((lane + j * LANES) << 19)
            first = (j * (neighbours // 8) + i) * 8
            keys_ref[first : first + 8, :] = jnp.where(sublane + 8 * i < count, key, DEAD)
    own = located(self_ref[...]) | ((sublane * LANES + lane) << 19)
    own = own | ((own_count_ref[...] - 20) << 14) | (1 << 13)
    keys_ref[neighbours * negatives // LANES :, :] = own[: negatives // LANES]


def owner_kernel(part_ref, ends_ref, lists_ref, message_hbm, self_hbm, *refs):
    outs = refs[: 4 * SIDE]
    table, stage, pick, rows, acc, offsets, places, ready, sems, place_sem, out_sems = refs[4 * SIDE :]
    items = message_hbm.shape[0]
    width = message_hbm.shape[1]
    tiles = width // LANES
    per_table = items // STAGE
    step = pl.program_id(0)
    devices = pl.num_programs(0)
    part = part_ref[0] * SIDE + part_ref[1]
    negatives = pick.shape[0]
    quarter = negatives // 4

    def asker(i):
        x = (part_ref[0] + i // SIDE) % SIDE
        y = (part_ref[1] + i % SIDE) % SIDE
        return x * SIDE + y

    def range_of(r):
        return jnp.where(part == 0, 0, ends_ref[r, jnp.maximum(part - 1, 0)]), ends_ref[r, part]

    def place_copy():
        return pltpu.make_async_copy(offsets, places, place_sem)

    def place(r, base):
        for c in range(BLOCK):
            line = lists_ref[r, pl.ds(base + c, 1), :]
            offsets[c : c + 1, :] = (line & 16383) * tiles
        place_copy().start()

    def stage_copy(c):
        source = message_hbm if c < per_table else self_hbm
        return pltpu.make_async_copy(
            source.at[pl.ds((c % per_table) * STAGE, STAGE), :], stage.at[c % 2], sems.at[c % 2]
        )

    def out_copy(slot, q, array, at):
        return pltpu.make_async_copy(
            ready.at[slot, pl.ds(q * quarter, quarter), :], array.at[at], out_sems.at[slot, q]
        )

    def wait_out(slot):
        for q in range(4):
            out_copy(slot, q, outs[0], 0).wait()

    @pl.when(step == 0)
    def _():
        stage_copy(0).start()
        offsets[...] = jnp.zeros_like(offsets)
        place(asker(0), range_of(asker(0))[0] >> 7)
        rows[...] = jnp.zeros_like(rows)
        for c in range(2 * per_table):
            if c + 1 < 2 * per_table:
                stage_copy(c + 1).start()
            stage_copy(c).wait()

            def spread(i, _, c=c):
                for u in range(4):
                    at = pl.multiple_of(i * 64 + u * 16, 16)
                    block = stage[c % 2, pl.ds(at, 16), :].astype(jnp.float32)
                    for half in range(2):
                        for j in range(tiles):
                            first = (c * STAGE + at + half * 8) * tiles + j
                            table[pl.ds(first, 8, stride=tiles), :] = block[
                                half * 8 : half * 8 + 8, j * LANES : (j + 1) * LANES
                            ]
                return 0

            lax.fori_loop(0, STAGE // 64, spread, 0)

    a = asker(step)
    start, end = range_of(a)
    row_first = start >> 7
    row_last = (end + 127) >> 7

    def picked(r):
        v = lax.broadcasted_iota(jnp.int32, (negatives, LANES), 0)
        line = lists_ref[a, pl.ds(r, 1), :]
        at = r * LANES + lax.broadcasted_iota(jnp.int32, (1, LANES), 1)
        who = jnp.where((at >= start) & (at < end), (line >> 19) & 511, -1)
        weight = jnp.where((line & 8192) != 0, ((line >> 14) & 31) + 20, 1).astype(jnp.float32)
        return jnp.where(v == who, weight, 0.0).astype(jnp.bfloat16)

    def gather(base):
        place_copy().wait()
        for c in range(BLOCK):
            r = base + c

            @pl.when(r < row_last)
            def _(c=c, r=r):
                pick[:, c * LANES : (c + 1) * LANES] = picked(r)
                for e in range(CHUNK):
                    at = pl.multiple_of(places[c, e], tiles)
                    rows[c, pl.ds(e, tiles, stride=STRIDE), :] = table[pl.ds(at, tiles), :]

            @pl.when(r >= row_last)
            def _(c=c):
                pick[:, c * LANES : (c + 1) * LANES] = jnp.zeros((negatives, LANES), jnp.bfloat16)

    def gather_more(base):
        place_copy().wait()

        def chunk(c, _):
            cols = pl.ds(pl.multiple_of(c * LANES, LANES), LANES)
            live = base + c < row_last
            pick[:, cols] = jnp.where(live, picked(base + c), 0).astype(jnp.bfloat16)

            def entry(e, _):
                at = pl.multiple_of(places[c, e], tiles)
                rows[c, pl.ds(e, tiles, stride=STRIDE), :] = table[pl.ds(at, tiles), :]
                return 0

            return lax.fori_loop(0, CHUNK, entry, 0)

        lax.fori_loop(0, BLOCK, chunk, 0)

    def summed():
        gathered = jnp.concatenate(
            [
                jnp.concatenate(
                    [rows[c, j * STRIDE : j * STRIDE + CHUNK, :].astype(jnp.bfloat16) for j in range(tiles)],
                    axis=1,
                )
                for c in range(BLOCK)
            ],
            axis=0,
        )
        return jnp.dot(pick[...], gathered, preferred_element_type=jnp.float32)

    gather(row_first)
    blocks = (row_last - row_first + BLOCK - 1) // BLOCK

    @pl.when((blocks <= 1) & (step + 1 < devices))
    def _():
        following = asker(step + 1)
        place(following, range_of(following)[0] >> 7)

    acc[...] = summed()

    @pl.when(blocks > 1)
    def _():
        def more(i, _):
            place(a, row_first + i * BLOCK)
            gather_more(row_first + i * BLOCK)
            acc[...] += summed()
            return 0

        lax.fori_loop(1, blocks, more, 0)

        @pl.when(step + 1 < devices)
        def _():
            following = asker(step + 1)
            place(following, range_of(following)[0] >> 7)

    slot = step % 2

    @pl.when(step >= 2)
    def _():
        wait_out(slot)

    ready[slot] = acc[...].astype(jnp.bfloat16)
    dx = step // SIDE
    dy = step % SIDE
    for d in range(SIDE):

        @pl.when(dx == d)
        def _(d=d):
            out_copy(slot, 0, outs[4 * d], dy).start()
            out_copy(slot, 1, outs[4 * d + 1], dy).start()

        @pl.when(dy == d)
        def _(d=d):
            out_copy(slot, 2, outs[4 * d + 2], dx).start()
            out_copy(slot, 3, outs[4 * d + 3], dx).start()

    @pl.when(step + 1 == devices)
    def _():
        wait_out(slot)
        wait_out(1 - slot)


def from_everyone(x, axis):
    devices = lax.axis_size(axis)
    return lax.all_to_all(jnp.broadcast_to(x[None], (devices, *x.shape)), axis, 0, 0, tiled=True)


def composed_keys(neighbour_slots, self_slot, neighbour_count, fetch_rows):
    negatives, neighbours = neighbour_slots.shape
    folded = negatives // LANES

    def tile_of(x):
        return jnp.pad(x.reshape(folded, LANES), ((0, 8 - folded), (0, 0)))

    return pl.pallas_call(
        compose_kernel,
        out_shape=jax.ShapeDtypeStruct(((neighbours + 1) * folded, LANES), jnp.int32),
        name="compose",
    )(
        neighbour_slots.T,
        tile_of(self_slot),
        neighbour_count[None, :],
        tile_of(neighbour_count),
        fetch_rows,
    )


def owner_sums(part, ends, lists, message_part, self_part, negatives):
    devices, lines, _ = lists.shape
    items, width = message_part.shape
    tiles = width // LANES
    quarter = jax.ShapeDtypeStruct((SIDE, negatives // 4, width), jnp.bfloat16)
    return pl.pallas_call(
        owner_kernel,
        grid=(devices,),
        in_specs=[
            pl.BlockSpec(memory_space=pltpu.SMEM),
            pl.BlockSpec(memory_space=pltpu.SMEM),
            pl.BlockSpec(memory_space=pltpu.VMEM),
            pl.BlockSpec(memory_space=pl.ANY),
            pl.BlockSpec(memory_space=pl.ANY),
        ],
        out_specs=[pl.BlockSpec(memory_space=pl.ANY)] * (4 * SIDE),
        out_shape=[quarter] * (4 * SIDE),
        scratch_shapes=[
            pltpu.VMEM((2 * items * tiles, LANES), jnp.float32),
            pltpu.VMEM((2, STAGE, width), jnp.bfloat16),
            pltpu.VMEM((negatives, BLOCK * CHUNK), jnp.bfloat16),
            pltpu.VMEM((BLOCK, tiles * STRIDE, LANES), jnp.float32),
            pltpu.VMEM((negatives, width), jnp.float32),
            pltpu.VMEM((16, LANES), jnp.int32),
            pltpu.SMEM((16, LANES), jnp.int32),
            pltpu.VMEM((2, negatives, width), jnp.bfloat16),
            pltpu.SemaphoreType.DMA((2,)),
            pltpu.SemaphoreType.DMA,
            pltpu.SemaphoreType.DMA((2, 4)),
        ],
        compiler_params=pltpu.CompilerParams(
            dimension_semantics=("arbitrary",), vmem_limit_bytes=60 * 2**20
        ),
        name="owner",
    )(part, ends, lists, message_part, self_part)


def moved(x, along, by):
    def place(i):
        x_at, y_at = divmod(i, SIDE)
        if along == "x":
            return (x_at + by) % SIDE * SIDE + y_at
        return x_at * SIDE + (y_at + by) % SIDE

    return lax.ppermute(x, "neg", [(i, place(i)) for i in range(SIDE * SIDE)])


def joined(*parts):
    return sum(p.astype(jnp.float32) for p in parts)


def ring_sums(first, second, along):
    far_up = moved(first[2], along, 1)
    far_down = moved(second[2], along, -1)
    near_up = moved(second[1], along, 1)
    near_down = moved(first[3], along, -1)
    sent_up = moved(joined(first[1], far_up).astype(jnp.bfloat16), along, 1)
    sent_down = moved(joined(second[3], far_down).astype(jnp.bfloat16), along, -1)
    return joined(first[0], sent_up, near_down), joined(second[0], near_up, sent_down)


def scattered_sums(outs):
    result = []
    for at, order in ((0, "xy"), (2, "yx")):
        first = [outs[4 * d + at] for d in range(SIDE)]
        second = [outs[4 * d + at + 1] for d in range(SIDE)]
        sums = ring_sums(first, second, order[0])
        cut = [[q[0]] + [q[d].astype(jnp.bfloat16) for d in range(1, SIDE)] for q in sums]
        result += ring_sums(cut[0], cut[1], order[1])
    return jnp.concatenate(result, axis=0)


def turned(x, deep, other):
    def place(i):
        z, core = divmod(i, 2)
        return (z + deep) % SIDE * 2 + (1 - core if other else core)

    return lax.ppermute(x, "qry", [(i, place(i)) for i in range(2 * SIDE)])


def all_queries(queries):
    up = turned(queries, 1, False)
    down = turned(queries, -1, False)
    far = turned(up, 1, False)
    mine = [queries, up, far, down]
    return mine + [turned(q, 0, True) for q in mine]


def per_device(
    items_table,
    fetch_rows,
    neighbour_slots,
    neighbour_count,
    self_slot,
    negative_count,
    message_weight,
    message_bias,
    self_weight,
    neighbour_weight,
    output_bias,
    queries,
):
    f32 = jnp.float32
    negatives = neighbour_count.shape[0]
    parts = lax.axis_size("neg")
    groups = lax.axis_size("qry")
    queries_all = jnp.concatenate(all_queries(queries), axis=0)

    keys = composed_keys(neighbour_slots, self_slot, neighbour_count, fetch_rows).reshape(-1)
    bounds = jnp.array([min((p + 1 - 8) << 28, DEAD) for p in range(parts)], jnp.int32)
    ends = jnp.sum((keys[None, :] < bounds[:, None]).astype(jnp.int32), axis=1)
    lines = jnp.concatenate([lax.sort(keys, is_stable=False), ends, jnp.zeros((184 * LANES - keys.size - parts,), jnp.int32)])
    lists = from_everyone(lines.reshape(184, LANES), "neg")

    message = jax.nn.relu(
        jnp.dot(items_table, message_weight, preferred_element_type=f32) + message_bias
    ).astype(jnp.bfloat16)
    message_part = jnp.dot(message, neighbour_weight, preferred_element_type=f32).astype(jnp.bfloat16)
    self_part = jnp.dot(items_table, self_weight, preferred_element_type=f32).astype(jnp.bfloat16)

    place = lax.axis_index("neg")
    part = jnp.stack([place // SIDE, place % SIDE]).astype(jnp.int32)
    outs = owner_sums(part, lists[:, keys.size // LANES, :parts], lists, message_part, self_part, negatives)
    total = scattered_sums(outs)

    hidden = jax.nn.relu(total / neighbour_count.astype(f32)[:, None] + output_bias)
    scale_inv = lax.rsqrt(jnp.mean(hidden * hidden, axis=-1, keepdims=True) + 0.25)
    negative_embed = (hidden * scale_inv).astype(jnp.bfloat16)

    own_count = lax.dynamic_slice(negative_count, (lax.axis_index("qry") * negatives,), (negatives,))
    log_count = jnp.log(own_count.astype(f32))
    scores = (
        0.25
        * lax.dot_general(negative_embed, queries_all, (((1,), (1,)), ((), ())), preferred_element_type=f32)
        - log_count[:, None]
    )
    peak = jnp.max(scores, axis=0)
    part_lse = peak + jnp.log(jnp.sum(jnp.exp(scores - peak[None, :]), axis=0))
    here = lax.axis_index("qry")
    z, core = here // 2, here % 2
    group = jnp.arange(groups)
    source = ((z - group // 2) % SIDE) + SIDE * ((group % 2) ^ core)
    picked = source[:, None] == group[None, :]
    blocks = part_lse.reshape(groups, -1)
    blocks = jnp.sum(jnp.where(picked[:, :, None], blocks[None], 0.0), axis=1)
    shared = jnp.broadcast_to(blocks[None], (parts, groups, queries.shape[0]))
    parts_lse = lax.all_to_all(
        shared.reshape(parts * groups, -1), ("neg", "qry"), split_axis=0, concat_axis=0, tiled=True
    )
    top = jnp.max(parts_lse, axis=0)
    query_lse = top + jnp.log(jnp.sum(jnp.exp(parts_lse - top[None, :]), axis=0))
    return (negative_embed, query_lse - math.log(negatives * parts * groups))


def solution(mesh):
    in_specs = (
        P("neg", None),
        P(("neg", "qry"), None),
        P(("neg", "qry"), None),
        P(("neg", "qry")),
        P(("neg", "qry")),
        P("neg"),
        P(),
        P(),
        P(),
        P(),
        P(),
        P("qry", None),
    )
    out_specs = (P(("neg", "qry"), None), P("qry"))
    return jax.shard_map(
        per_device, mesh=mesh, in_specs=in_specs, out_specs=out_specs, check_vma=False
    )
```

```python
import functools
import math

import jax
import jax.numpy as jnp
from jax import lax
from jax.experimental import pallas as pl
from jax.experimental.pallas import tpu as pltpu
from jax.sharding import PartitionSpec as P

LANES = 128
DEAD = 2**31 - 1
CHUNK = 128
STRIDE = 132
BLOCK = 10
STAGE = 1024
SIDE = 4
SCORED = 256
MESSAGES = 6
WHERE = {
    (0, 0): (0, 0),
    (1, 0): (1, 0),
    (0, 2): (2, 0),
    (1, 1): (2, SIDE),
    (1, 2): (3, 0),
    (0, 3): (3, SIDE),
    (0, 1): (4, 0),
    (1, 3): (5, 0),
}


def compose_kernel(slots_ref, self_ref, count_ref, fetch_ref, keys_ref):
    neighbours, negatives = slots_ref.shape
    parts, per_part = fetch_ref.shape
    per_line = per_part // LANES
    half = parts // 2
    packed = fetch_ref[:half, :] | (fetch_ref[half:, :] << 13)
    lines = [
        jnp.broadcast_to(packed[p : p + 1, j * LANES : (j + 1) * LANES], (8, LANES))
        for p in range(half)
        for j in range(per_line)
    ]

    def located(slot):
        hi = slot >> 7
        lo = slot & 127
        upper = hi >= len(lines)
        folded = jnp.where(upper, hi - len(lines), hi)
        found = jnp.zeros_like(slot)
        for h, line in enumerate(lines):
            at = jnp.take_along_axis(line, lo, axis=1, mode="promise_in_bounds")
            found = jnp.where(folded == h, at, found)
        row = jnp.where(upper, found >> 13, found & 8191)
        return ((((hi * 205) >> 10) - 8) << 28) | row

    sublane = lax.broadcasted_iota(jnp.int32, (8, LANES), 0)
    lane = lax.broadcasted_iota(jnp.int32, (8, LANES), 1)
    for j in range(negatives // LANES):
        cols = slice(j * LANES, (j + 1) * LANES)
        count = jnp.broadcast_to(count_ref[:, cols], (8, LANES))
        for i in range(neighbours // 8):
            key = located(slots_ref[8 * i : 8 * (i + 1), cols]) | ((lane + j * LANES) << 19)
            first = (j * (neighbours // 8) + i) * 8
            keys_ref[first : first + 8, :] = jnp.where(sublane + 8 * i < count, key, DEAD)

    def tile_of(ref):
        tiles = [ref[:, j * LANES : (j + 1) * LANES] for j in range(negatives // LANES)]
        return jnp.concatenate(tiles + [jnp.zeros((8 - len(tiles), LANES), jnp.int32)], axis=0)

    own = located(tile_of(self_ref)) | ((sublane * LANES + lane) << 19)
    own = own | ((tile_of(count_ref) - 20) << 14) | (1 << 13)
    keys_ref[neighbours * negatives // LANES :, :] = own[: negatives // LANES]


def owner_kernel(part_ref, ends_ref, lists_ref, message_hbm, self_hbm, *refs):
    outs = refs[: 2 * MESSAGES]
    table, stage, pick, rows, acc, offsets, places, ready, sems, place_sem, out_sems = refs[2 * MESSAGES :]
    items = message_hbm.shape[0]
    width = message_hbm.shape[1]
    tiles = width // LANES
    per_table = items // STAGE
    step = pl.program_id(0)
    devices = pl.num_programs(0)
    part = part_ref[0] * SIDE + part_ref[1]
    negatives = pick.shape[0]
    quarter = negatives // 4

    def asker(i):
        x = (part_ref[0] + i // SIDE) % SIDE
        y = (part_ref[1] + i % SIDE) % SIDE
        return x * SIDE + y

    def range_of(r):
        return jnp.where(part == 0, 0, ends_ref[r, jnp.maximum(part - 1, 0)]), ends_ref[r, part]

    def place_copy():
        return pltpu.make_async_copy(offsets, places, place_sem)

    def place(r, base):
        for c in range(BLOCK):
            line = lists_ref[r, pl.ds(base + c, 1), :]
            offsets[c : c + 1, :] = (line & 16383) * tiles
        place_copy().start()

    def stage_copy(c):
        source = message_hbm if c < per_table else self_hbm
        return pltpu.make_async_copy(
            source.at[pl.ds((c % per_table) * STAGE, STAGE), :], stage.at[c % 2], sems.at[c % 2]
        )

    def out_copy(slot, q, array, at):
        return pltpu.make_async_copy(
            ready.at[slot, pl.ds(q * quarter, quarter), :], array.at[at], out_sems.at[slot, q]
        )

    def wait_out(slot):
        for q in range(4):
            out_copy(slot, q, outs[0], 0).wait()

    @pl.when(step == 0)
    def _():
        stage_copy(0).start()
        offsets[...] = jnp.zeros_like(offsets)
        place(asker(0), range_of(asker(0))[0] >> 7)
        rows[...] = jnp.zeros_like(rows)
        for c in range(2 * per_table):
            if c + 1 < 2 * per_table:
                stage_copy(c + 1).start()
            stage_copy(c).wait()

            def spread(i, _, c=c):
                for u in range(4):
                    at = pl.multiple_of(i * 64 + u * 16, 16)
                    block = stage[c % 2, pl.ds(at, 16), :].astype(jnp.float32)
                    for half in range(2):
                        for j in range(tiles):
                            first = (c * STAGE + at + half * 8) * tiles + j
                            table[pl.ds(first, 8, stride=tiles), :] = block[
                                half * 8 : half * 8 + 8, j * LANES : (j + 1) * LANES
                            ]
                return 0

            lax.fori_loop(0, STAGE // 64, spread, 0)

    a = asker(step)
    start, end = range_of(a)
    row_first = start >> 7
    row_last = (end + 127) >> 7

    def picked(r):
        v = lax.broadcasted_iota(jnp.int32, (negatives, LANES), 0)
        line = lists_ref[a, pl.ds(r, 1), :]
        at = r * LANES + lax.broadcasted_iota(jnp.int32, (1, LANES), 1)
        who = jnp.where((at >= start) & (at < end), (line >> 19) & 511, -1)
        weight = jnp.where((line & 8192) != 0, ((line >> 14) & 31) + 20, 1).astype(jnp.float32)
        return jnp.where(v == who, weight, 0.0).astype(jnp.bfloat16)

    def gather(base):
        place_copy().wait()
        for c in range(BLOCK):
            r = base + c

            @pl.when(r < row_last)
            def _(c=c, r=r):
                pick[:, c * LANES : (c + 1) * LANES] = picked(r)
                for e in range(CHUNK):
                    at = pl.multiple_of(places[c, e], tiles)
                    rows[c, pl.ds(e, tiles, stride=STRIDE), :] = table[pl.ds(at, tiles), :]

            @pl.when(r >= row_last)
            def _(c=c):
                pick[:, c * LANES : (c + 1) * LANES] = jnp.zeros((negatives, LANES), jnp.bfloat16)

    def gather_more(base):
        place_copy().wait()

        def chunk(c, _):
            cols = pl.ds(pl.multiple_of(c * LANES, LANES), LANES)
            live = base + c < row_last
            pick[:, cols] = jnp.where(live, picked(base + c), 0).astype(jnp.bfloat16)

            def entry(e, _):
                at = pl.multiple_of(places[c, e], tiles)
                rows[c, pl.ds(e, tiles, stride=STRIDE), :] = table[pl.ds(at, tiles), :]
                return 0

            return lax.fori_loop(0, CHUNK, entry, 0)

        lax.fori_loop(0, BLOCK, chunk, 0)

    def summed():
        gathered = jnp.concatenate(
            [
                jnp.concatenate(
                    [rows[c, j * STRIDE : j * STRIDE + CHUNK, :].astype(jnp.bfloat16) for j in range(tiles)],
                    axis=1,
                )
                for c in range(BLOCK)
            ],
            axis=0,
        )
        return jnp.dot(pick[...], gathered, preferred_element_type=jnp.float32)

    gather(row_first)
    blocks = (row_last - row_first + BLOCK - 1) // BLOCK

    @pl.when((blocks <= 1) & (step + 1 < devices))
    def _():
        following = asker(step + 1)
        place(following, range_of(following)[0] >> 7)

    acc[...] = summed()

    @pl.when(blocks > 1)
    def _():
        def more(i, _):
            place(a, row_first + i * BLOCK)
            gather_more(row_first + i * BLOCK)
            acc[...] += summed()
            return 0

        lax.fori_loop(1, blocks, more, 0)

        @pl.when(step + 1 < devices)
        def _():
            following = asker(step + 1)
            place(following, range_of(following)[0] >> 7)

    slot = step % 2

    @pl.when(step >= 2)
    def _():
        wait_out(slot)

    ready[slot] = acc[...].astype(jnp.bfloat16)
    dx = step // SIDE
    dy = step % SIDE
    for d in range(SIDE):

        @pl.when(dx == d)
        def _(d=d):
            for h in range(2):
                array, first = WHERE[h, d]
                out_copy(slot, h, outs[array], first + dy).start()

        @pl.when(dy == d)
        def _(d=d):
            for h in range(2):
                array, first = WHERE[h, d]
                out_copy(slot, 2 + h, outs[MESSAGES + array], first + dx).start()

    @pl.when(step + 1 == devices)
    def _():
        wait_out(slot)
        wait_out(1 - slot)


def from_everyone(x, axis):
    devices = lax.axis_size(axis)
    return lax.all_to_all(jnp.broadcast_to(x[None], (devices, *x.shape)), axis, 0, 0, tiled=True)


def composed_keys(neighbour_slots, self_slot, neighbour_count, fetch_rows):
    negatives, neighbours = neighbour_slots.shape
    folded = negatives // LANES
    return pl.pallas_call(
        compose_kernel,
        out_shape=jax.ShapeDtypeStruct(((neighbours + 1) * folded, LANES), jnp.int32),
        name="compose",
    )(
        neighbour_slots.T,
        self_slot[None, :],
        neighbour_count[None, :],
        fetch_rows,
    )


def owner_sums(part, ends, lists, message_part, self_part, negatives):
    devices, lines, _ = lists.shape
    items, width = message_part.shape
    tiles = width // LANES
    quarter = [
        jax.ShapeDtypeStruct((deep * SIDE, negatives // 4, width), jnp.bfloat16) for deep in (1, 1, 2, 2, 1, 1)
    ]
    return pl.pallas_call(
        owner_kernel,
        grid=(devices,),
        in_specs=[
            pl.BlockSpec(memory_space=pltpu.SMEM),
            pl.BlockSpec(memory_space=pltpu.SMEM),
            pl.BlockSpec(memory_space=pltpu.VMEM),
            pl.BlockSpec(memory_space=pl.ANY),
            pl.BlockSpec(memory_space=pl.ANY),
        ],
        out_specs=[pl.BlockSpec(memory_space=pl.ANY)] * (2 * MESSAGES),
        out_shape=quarter * 2,
        scratch_shapes=[
            pltpu.VMEM((2 * items * tiles, LANES), jnp.float32),
            pltpu.VMEM((2, STAGE, width), jnp.bfloat16),
            pltpu.VMEM((negatives, BLOCK * CHUNK), jnp.bfloat16),
            pltpu.VMEM((BLOCK, tiles * STRIDE, LANES), jnp.float32),
            pltpu.VMEM((negatives, width), jnp.float32),
            pltpu.VMEM((16, LANES), jnp.int32),
            pltpu.SMEM((16, LANES), jnp.int32),
            pltpu.VMEM((2, negatives, width), jnp.bfloat16),
            pltpu.SemaphoreType.DMA((2,)),
            pltpu.SemaphoreType.DMA,
            pltpu.SemaphoreType.DMA((2, 4)),
        ],
        compiler_params=pltpu.CompilerParams(
            dimension_semantics=("arbitrary",), vmem_limit_bytes=60 * 2**20
        ),
        name="owner",
    )(part, ends, lists, message_part, self_part)


def moved(x, along, by):
    def place(i):
        x_at, y_at = divmod(i, SIDE)
        if along == "x":
            return (x_at + by) % SIDE * SIDE + y_at
        return x_at * SIDE + (y_at + by) % SIDE

    return lax.ppermute(x, "neg", [(i, place(i)) for i in range(SIDE * SIDE)])


def joined(*parts):
    return sum(p.astype(jnp.float32) for p in parts)


def ring_sums(own_first, own_second, up, down, next_up, next_down, along):
    half = up.shape[0] // 2
    came_up = moved(up, along, 1)
    came_down = moved(down, along, -1)
    sent_up = moved(joined(next_up, came_up[:half]).astype(jnp.bfloat16), along, 1)
    sent_down = moved(joined(next_down, came_down[:half]).astype(jnp.bfloat16), along, -1)
    return joined(own_first, sent_up, came_down[half:]), joined(own_second, came_up[half:], sent_down)


def scattered_sums(outs):
    result = []
    for at, order in ((0, "xy"), (MESSAGES, "yx")):
        first, second = ring_sums(*outs[at : at + MESSAGES], order[0])
        low_first, low_second = first.astype(jnp.bfloat16), second.astype(jnp.bfloat16)
        up = jnp.concatenate([low_first[2:3], low_second[1:2]], axis=0)
        down = jnp.concatenate([low_second[2:3], low_first[3:4]], axis=0)
        result += ring_sums(
            first[0:1], second[0:1], up, down, low_first[1:2], low_second[3:4], order[1]
        )
    return result


def turned(x, deep, other):
    def place(i):
        z, core = divmod(i, 2)
        return (z + deep) % SIDE * 2 + (1 - core if other else core)

    return lax.ppermute(x, "qry", [(i, place(i)) for i in range(2 * SIDE)])


def all_queries(queries):
    up = turned(queries, 1, False)
    down = turned(queries, -1, False)
    far = turned(up, 1, False)
    mine = [queries, up, far, down]
    return mine + [turned(q, 0, True) for q in mine]


def table_kernel(items_ref, message_ref, bias_ref, neighbour_ref, self_ref, message_out, self_out):
    f32 = jnp.float32
    items = items_ref[...]
    message = jnp.dot(items, message_ref[...], preferred_element_type=f32) + bias_ref[...]
    message = jnp.maximum(message, 0.0).astype(jnp.bfloat16)
    message_out[...] = jnp.dot(message, neighbour_ref[...], preferred_element_type=f32).astype(jnp.bfloat16)
    self_out[...] = jnp.dot(items, self_ref[...], preferred_element_type=f32).astype(jnp.bfloat16)


def tables(items_table, message_weight, message_bias, neighbour_weight, self_weight):
    items, width = items_table.shape
    weight = pl.BlockSpec((width, width), lambda i: (0, 0))
    block = pl.BlockSpec((STAGE, width), lambda i: (i, 0))
    return pl.pallas_call(
        table_kernel,
        grid=(items // STAGE,),
        in_specs=[block, weight, pl.BlockSpec((1, width), lambda i: (0, 0)), weight, weight],
        out_specs=[block, block],
        out_shape=[jax.ShapeDtypeStruct((items, width), jnp.bfloat16)] * 2,
        compiler_params=pltpu.CompilerParams(dimension_semantics=("arbitrary",)),
        name="tables",
    )(items_table, message_weight, message_bias[None, :], neighbour_weight, self_weight)


def score_kernel(*refs):
    sums = refs[:4]
    count_ref, bias_ref, log_ref = refs[4:7]
    queries = refs[7 : 7 + 2 * SIDE]
    embed_ref, lse_ref, held, sems = refs[7 + 2 * SIDE :]
    f32 = jnp.float32
    rows = queries[0].shape[0]

    def copy(j, source):
        return pltpu.make_async_copy(source, held.at[pl.ds(j * rows, rows), :], sems.at[j])

    for j, source in enumerate(queries):
        copy(j, source).start()
    quarter = embed_ref.shape[0] // 4
    for q in range(4):
        at = slice(q * quarter, (q + 1) * quarter)
        hidden = jnp.maximum(sums[q][...] / count_ref[at, :] + bias_ref[...], 0.0)
        scale_inv = lax.rsqrt(jnp.mean(hidden * hidden, axis=-1, keepdims=True) + 0.25)
        embed_ref[at, :] = (hidden * scale_inv).astype(jnp.bfloat16)

    def block(j, _):
        copy(j, queries[0]).wait()

        def pair(i, _):
            first = j * rows + i * 2 * SCORED
            for u in range(2):
                at = pl.multiple_of(first + u * SCORED, SCORED)
                scores = lax.dot_general(
                    embed_ref[...], held[pl.ds(at, SCORED), :], (((1,), (1,)), ((), ())), preferred_element_type=f32
                )
                scores = 0.25 * scores - log_ref[...]
                peak = jnp.max(scores, axis=0, keepdims=True)
                total = jnp.sum(jnp.exp(scores - peak), axis=0, keepdims=True)
                lse_ref[pl.ds(at // SCORED, 1), :] = peak + jnp.log(total)
            return 0

        return lax.fori_loop(0, rows // (2 * SCORED), pair, 0)

    lax.fori_loop(0, len(queries), block, 0)


def scored(sums, count, bias, log_count, queries):
    negatives = count.shape[0]
    rows, width = queries[0].shape
    total = rows * len(queries)
    in_vmem = pl.BlockSpec(memory_space=pltpu.VMEM)
    return pl.pallas_call(
        score_kernel,
        in_specs=[in_vmem] * 7 + [pl.BlockSpec(memory_space=pl.ANY)] * len(queries),
        out_specs=[in_vmem] * 2,
        out_shape=[
            jax.ShapeDtypeStruct((negatives, width), jnp.bfloat16),
            jax.ShapeDtypeStruct((total // SCORED, SCORED), jnp.float32),
        ],
        scratch_shapes=[
            pltpu.VMEM((total, width), jnp.bfloat16),
            pltpu.SemaphoreType.DMA((len(queries),)),
        ],
        name="score",
    )(*sums, count[:, None], bias[None, :], log_count[:, None], *queries)


def per_device(
    items_table,
    fetch_rows,
    neighbour_slots,
    neighbour_count,
    self_slot,
    negative_count,
    message_weight,
    message_bias,
    self_weight,
    neighbour_weight,
    output_bias,
    queries,
):
    f32 = jnp.float32
    negatives = neighbour_count.shape[0]
    parts = lax.axis_size("neg")
    groups = lax.axis_size("qry")
    query_blocks = all_queries(queries)

    keys = composed_keys(neighbour_slots, self_slot, neighbour_count, fetch_rows).reshape(-1)
    bounds = jnp.array([min((p + 1 - 8) << 28, DEAD) for p in range(parts)], jnp.int32)
    ends = jnp.sum((keys[None, :] < bounds[:, None]).astype(jnp.int32), axis=1)
    lines = jnp.concatenate([lax.sort(keys, is_stable=False), ends, jnp.zeros((184 * LANES - keys.size - parts,), jnp.int32)])
    lists = from_everyone(lines.reshape(184, LANES), "neg")

    message_part, self_part = tables(items_table, message_weight, message_bias, neighbour_weight, self_weight)

    place = lax.axis_index("neg")
    part = jnp.stack([place // SIDE, place % SIDE]).astype(jnp.int32)
    outs = owner_sums(part, lists[:, keys.size // LANES, :parts], lists, message_part, self_part, negatives)
    sums = [q[0] for q in scattered_sums(outs)]

    own_count = lax.dynamic_slice(negative_count, (lax.axis_index("qry") * negatives,), (negatives,))
    log_count = jnp.log(own_count.astype(f32))
    negative_embed, part_lse = scored(sums, neighbour_count.astype(f32), output_bias, log_count, query_blocks)
    here = lax.axis_index("qry")
    z, core = here // 2, here % 2
    group = jnp.arange(groups)
    source = ((z - group // 2) % SIDE) + SIDE * ((group % 2) ^ core)
    picked = source[:, None] == group[None, :]
    blocks = part_lse.reshape(groups, -1)
    blocks = jnp.sum(jnp.where(picked[:, :, None], blocks[None], 0.0), axis=1)
    shared = jnp.broadcast_to(blocks[None], (parts, groups, queries.shape[0]))
    parts_lse = lax.all_to_all(
        shared.reshape(parts * groups, -1), ("neg", "qry"), split_axis=0, concat_axis=0, tiled=True
    )
    top = jnp.max(parts_lse, axis=0)
    query_lse = top + jnp.log(jnp.sum(jnp.exp(parts_lse - top[None, :]), axis=0))
    return (negative_embed, query_lse - math.log(negatives * parts * groups))


def solution(mesh):
    in_specs = (
        P("neg", None),
        P(("neg", "qry"), None),
        P(("neg", "qry"), None),
        P(("neg", "qry")),
        P(("neg", "qry")),
        P("neg"),
        P(),
        P(),
        P(),
        P(),
        P(),
        P("qry", None),
    )
    out_specs = (P(("neg", "qry"), None), P("qry"))
    return jax.shard_map(
        per_device, mesh=mesh, in_specs=in_specs, out_specs=out_specs, check_vma=False
    )
```

```python
import math

import jax
import jax.numpy as jnp
from jax import lax
from jax.experimental import pallas as pl
from jax.experimental.pallas import tpu as pltpu
from jax.sharding import PartitionSpec as P


LANES = 128
DEAD = 2**31 - 1
CHUNK = 128
STRIDE = 132
BLOCK = 10
STAGE = 1024
DEEP = 4
SIDE = 4
SCORED = 256
MESSAGES = 2 * SIDE


def compose_kernel(slots_ref, self_ref, count_ref, fetch_ref, keys_ref):
    neighbours, negatives = slots_ref.shape
    parts, per_part = fetch_ref.shape
    per_line = per_part // LANES
    half = parts // 2
    packed = fetch_ref[:half, :] | (fetch_ref[half:, :] << 13)
    lines = [
        jnp.broadcast_to(packed[p : p + 1, j * LANES : (j + 1) * LANES], (8, LANES))
        for p in range(half)
        for j in range(per_line)
    ]

    def located(slot):
        hi = slot >> 7
        lo = slot & 127
        upper = hi >= len(lines)
        folded = jnp.where(upper, hi - len(lines), hi)
        found = jnp.zeros_like(slot)
        for h, line in enumerate(lines):
            at = jnp.take_along_axis(line, lo, axis=1, mode="promise_in_bounds")
            found = jnp.where(folded == h, at, found)
        row = jnp.where(upper, found >> 13, found & 8191)
        return ((((hi * 205) >> 10) - 8) << 28) | row

    sublane = lax.broadcasted_iota(jnp.int32, (8, LANES), 0)
    lane = lax.broadcasted_iota(jnp.int32, (8, LANES), 1)
    for j in range(negatives // LANES):
        cols = slice(j * LANES, (j + 1) * LANES)
        count = jnp.broadcast_to(count_ref[:, cols], (8, LANES))
        for i in range(neighbours // 8):
            key = located(slots_ref[8 * i : 8 * (i + 1), cols]) | ((lane + j * LANES) << 19)
            first = (j * (neighbours // 8) + i) * 8
            keys_ref[first : first + 8, :] = jnp.where(sublane + 8 * i < count, key, DEAD)

    def tile_of(ref):
        tiles = [ref[:, j * LANES : (j + 1) * LANES] for j in range(negatives // LANES)]
        return jnp.concatenate(tiles + [jnp.zeros((8 - len(tiles), LANES), jnp.int32)], axis=0)

    own = located(tile_of(self_ref)) | ((sublane * LANES + lane) << 19)
    own = own | ((tile_of(count_ref) - 20) << 14) | (1 << 13)
    keys_ref[neighbours * negatives // LANES :, :] = own[: negatives // LANES]


def owner_kernel(part_ref, ends_ref, lists_ref, message_hbm, self_hbm, *refs):
    outs = refs[: 2 * MESSAGES]
    table, stage, pick, rows, acc, offsets, places, ready, sems, place_sem, out_sems = refs[2 * MESSAGES :]
    items = message_hbm.shape[0]
    width = message_hbm.shape[1]
    tiles = width // LANES
    per_table = items // STAGE
    step = pl.program_id(0)
    devices = pl.num_programs(0)
    part = part_ref[0] * SIDE + part_ref[1]
    negatives = pick.shape[0]
    quarter = negatives // 4

    def asker(i):
        x = (part_ref[0] + i // SIDE) % SIDE
        y = (part_ref[1] + i % SIDE) % SIDE
        return x * SIDE + y

    def range_of(r):
        return jnp.where(part == 0, 0, ends_ref[r, jnp.maximum(part - 1, 0)]), ends_ref[r, part]

    def place_copy():
        return pltpu.make_async_copy(offsets, places, place_sem)

    def place(r, base):
        for c in range(BLOCK):
            line = lists_ref[r, pl.ds(base + c, 1), :]
            offsets[c : c + 1, :] = (line & 16383) * tiles
        place_copy().start()

    def stage_copy(c):
        source = message_hbm if c < per_table else self_hbm
        return pltpu.make_async_copy(
            source.at[pl.ds((c % per_table) * STAGE, STAGE), :], stage.at[c % DEEP], sems.at[c % DEEP]
        )

    def out_copy(slot, q, array, at):
        return pltpu.make_async_copy(
            ready.at[slot, pl.ds(q * quarter, quarter), :], array.at[at], out_sems.at[slot, q]
        )

    def wait_out(slot):
        for q in range(4):
            out_copy(slot, q, outs[0], 0).wait()

    @pl.when(step == 0)
    def _():
        for c in range(DEEP):
            stage_copy(c).start()
        offsets[...] = jnp.zeros_like(offsets)
        place(asker(0), range_of(asker(0))[0] >> 7)
        rows[...] = jnp.zeros_like(rows)
        for c in range(2 * per_table):
            stage_copy(c).wait()

            def spread(i, _, c=c):
                for u in range(4):
                    at = pl.multiple_of(i * 64 + u * 16, 16)
                    block = stage[c % DEEP, pl.ds(at, 16), :].astype(jnp.float32)
                    for half in range(2):
                        for j in range(tiles):
                            first = (c * STAGE + at + half * 8) * tiles + j
                            table[pl.ds(first, 8, stride=tiles), :] = block[
                                half * 8 : half * 8 + 8, j * LANES : (j + 1) * LANES
                            ]
                return 0

            lax.fori_loop(0, STAGE // 64, spread, 0)
            if c + DEEP < 2 * per_table:
                stage_copy(c + DEEP).start()

    a = asker(step)
    start, end = range_of(a)
    row_first = start >> 7
    row_last = (end + 127) >> 7

    def picked(r):
        v = lax.broadcasted_iota(jnp.int32, (negatives, LANES), 0)
        line = lists_ref[a, pl.ds(r, 1), :]
        at = r * LANES + lax.broadcasted_iota(jnp.int32, (1, LANES), 1)
        who = jnp.where((at >= start) & (at < end), (line >> 19) & 511, -1)
        weight = jnp.where((line & 8192) != 0, ((line >> 14) & 31) + 20, 1).astype(jnp.float32)
        return jnp.where(v == who, weight, 0.0).astype(jnp.bfloat16)

    def gather(base):
        place_copy().wait()
        for c in range(BLOCK):
            r = base + c

            @pl.when(r < row_last)
            def _(c=c, r=r):
                pick[:, c * LANES : (c + 1) * LANES] = picked(r)
                for e in range(CHUNK):
                    at = pl.multiple_of(places[c, e], tiles)
                    rows[c, pl.ds(e, tiles, stride=STRIDE), :] = table[pl.ds(at, tiles), :]

            @pl.when(r >= row_last)
            def _(c=c):
                pick[:, c * LANES : (c + 1) * LANES] = jnp.zeros((negatives, LANES), jnp.bfloat16)

    def gather_more(base):
        place_copy().wait()

        def chunk(c, _):
            cols = pl.ds(pl.multiple_of(c * LANES, LANES), LANES)
            live = base + c < row_last
            pick[:, cols] = jnp.where(live, picked(base + c), 0).astype(jnp.bfloat16)

            def entry(e, _):
                at = pl.multiple_of(places[c, e], tiles)
                rows[c, pl.ds(e, tiles, stride=STRIDE), :] = table[pl.ds(at, tiles), :]
                return 0

            return lax.fori_loop(0, CHUNK, entry, 0)

        lax.fori_loop(0, BLOCK, chunk, 0)

    def summed():
        gathered = jnp.concatenate(
            [
                jnp.concatenate(
                    [rows[c, j * STRIDE : j * STRIDE + CHUNK, :].astype(jnp.bfloat16) for j in range(tiles)],
                    axis=1,
                )
                for c in range(BLOCK)
            ],
            axis=0,
        )
        return jnp.dot(pick[...], gathered, preferred_element_type=jnp.float32)

    gather(row_first)
    blocks = (row_last - row_first + BLOCK - 1) // BLOCK

    @pl.when((blocks <= 1) & (step + 1 < devices))
    def _():
        following = asker(step + 1)
        place(following, range_of(following)[0] >> 7)

    acc[...] = summed()

    @pl.when(blocks > 1)
    def _():
        def more(i, _):
            place(a, row_first + i * BLOCK)
            gather_more(row_first + i * BLOCK)
            acc[...] += summed()
            return 0

        lax.fori_loop(1, blocks, more, 0)

        @pl.when(step + 1 < devices)
        def _():
            following = asker(step + 1)
            place(following, range_of(following)[0] >> 7)

    slot = step % 2

    @pl.when(step >= 2)
    def _():
        wait_out(slot)

    ready[slot] = acc[...].astype(jnp.bfloat16)
    dx = step // SIDE
    dy = step % SIDE
    for d in range(SIDE):

        @pl.when(dx == d)
        def _(d=d):
            for h in range(2):
                out_copy(slot, h, outs[2 * d + h], dy).start()

        @pl.when(dy == d)
        def _(d=d):
            for h in range(2):
                out_copy(slot, 2 + h, outs[MESSAGES + 2 * d + h], dx).start()

    @pl.when(step + 1 == devices)
    def _():
        wait_out(slot)
        wait_out(1 - slot)


def from_everyone(x, axis):
    devices = lax.axis_size(axis)
    return lax.all_to_all(jnp.broadcast_to(x[None], (devices, *x.shape)), axis, 0, 0, tiled=True)


def composed_keys(neighbour_slots, self_slot, neighbour_count, fetch_rows):
    negatives, neighbours = neighbour_slots.shape
    folded = negatives // LANES
    return pl.pallas_call(
        compose_kernel,
        out_shape=jax.ShapeDtypeStruct(((neighbours + 1) * folded, LANES), jnp.int32),
        name="compose",
    )(
        neighbour_slots.T,
        self_slot[None, :],
        neighbour_count[None, :],
        fetch_rows,
    )


def owner_sums(part, ends, lists, message_part, self_part, negatives):
    devices, _, _ = lists.shape
    items, width = message_part.shape
    tiles = width // LANES
    quarter = [jax.ShapeDtypeStruct((SIDE, negatives // 4, width), jnp.bfloat16)]
    return pl.pallas_call(
        owner_kernel,
        grid=(devices,),
        in_specs=[
            pl.BlockSpec(memory_space=pltpu.SMEM),
            pl.BlockSpec(memory_space=pltpu.SMEM),
            pl.BlockSpec(memory_space=pltpu.VMEM),
            pl.BlockSpec(memory_space=pl.ANY),
            pl.BlockSpec(memory_space=pl.ANY),
        ],
        out_specs=[pl.BlockSpec(memory_space=pl.ANY)] * (2 * MESSAGES),
        out_shape=quarter * (2 * MESSAGES),
        scratch_shapes=[
            pltpu.VMEM((2 * items * tiles, LANES), jnp.float32),
            pltpu.VMEM((DEEP, STAGE, width), jnp.bfloat16),
            pltpu.VMEM((negatives, BLOCK * CHUNK), jnp.bfloat16),
            pltpu.VMEM((BLOCK, tiles * STRIDE, LANES), jnp.float32),
            pltpu.VMEM((negatives, width), jnp.float32),
            pltpu.VMEM((16, LANES), jnp.int32),
            pltpu.SMEM((16, LANES), jnp.int32),
            pltpu.VMEM((2, negatives, width), jnp.bfloat16),
            pltpu.SemaphoreType.DMA((DEEP,)),
            pltpu.SemaphoreType.DMA,
            pltpu.SemaphoreType.DMA((2, 4)),
        ],
        compiler_params=pltpu.CompilerParams(
            dimension_semantics=("arbitrary",), vmem_limit_bytes=60 * 2**20
        ),
        name="owner",
    )(part, ends, lists, message_part, self_part)


def moved(x, along, by):
    def place(i):
        x_at, y_at = divmod(i, SIDE)
        if along == "x":
            return (x_at + by) % SIDE * SIDE + y_at
        return x_at * SIDE + (y_at + by) % SIDE

    return lax.ppermute(x, "neg", [(i, place(i)) for i in range(SIDE * SIDE)])


def joined(*parts):
    return sum(p.astype(jnp.float32) for p in parts)


def ring_sums(parts, along):
    far_up = moved(parts[2][0], along, 1)
    far_down = moved(parts[2][1], along, -1)
    near_up = moved(parts[1][1], along, 1)
    near_down = moved(parts[3][0], along, -1)
    sent_up = moved(joined(parts[1][0], far_up).astype(jnp.bfloat16), along, 1)
    sent_down = moved(joined(parts[3][1], far_down).astype(jnp.bfloat16), along, -1)
    return joined(parts[0][0], sent_up, near_down), joined(parts[0][1], near_up, sent_down)


def joint_sums(own_first, own_second, up, down, next_up, next_down, along):
    half = up.shape[0] // 2
    came_up = moved(up, along, 1)
    came_down = moved(down, along, -1)
    sent_up = moved(joined(next_up, came_up[:half]).astype(jnp.bfloat16), along, 1)
    sent_down = moved(joined(next_down, came_down[:half]).astype(jnp.bfloat16), along, -1)
    return joined(own_first, sent_up, came_down[half:]), joined(own_second, came_up[half:], sent_down)


def scattered_sums(outs):
    result = []
    for at, order in ((0, "xy"), (MESSAGES, "yx")):
        parts = [outs[at + 2 * d : at + 2 * d + 2] for d in range(SIDE)]
        first, second = ring_sums(parts, order[0])
        low_first, low_second = first.astype(jnp.bfloat16), second.astype(jnp.bfloat16)
        up = jnp.concatenate([low_first[2:3], low_second[1:2]], axis=0)
        down = jnp.concatenate([low_second[2:3], low_first[3:4]], axis=0)
        result += joint_sums(first[0:1], second[0:1], up, down, low_first[1:2], low_second[3:4], order[1])
    return result


def turned(x, deep, other):
    def place(i):
        z, core = divmod(i, 2)
        return (z + deep) % SIDE * 2 + (1 - core if other else core)

    return lax.ppermute(x, "qry", [(i, place(i)) for i in range(2 * SIDE)])


def all_queries(queries):
    up = turned(queries, 1, False)
    down = turned(queries, -1, False)
    other = turned(queries, 0, True)
    far = turned(up, 1, False)
    other_up = turned(up, 0, True)
    other_down = turned(down, 0, True)
    other_far = turned(far, 0, True)
    return [queries, up, far, down, other, other_up, other_far, other_down]


def table_kernel(items_ref, message_ref, bias_ref, neighbour_ref, self_ref, message_out, self_out):
    f32 = jnp.float32
    items = items_ref[...]
    message = jnp.dot(items, message_ref[...], preferred_element_type=f32) + bias_ref[...]
    message = jnp.maximum(message, 0.0).astype(jnp.bfloat16)
    message_out[...] = jnp.dot(message, neighbour_ref[...], preferred_element_type=f32).astype(jnp.bfloat16)
    self_out[...] = jnp.dot(items, self_ref[...], preferred_element_type=f32).astype(jnp.bfloat16)


def tables(items_table, message_weight, message_bias, neighbour_weight, self_weight):
    items, width = items_table.shape
    weight = pl.BlockSpec((width, width), lambda i: (0, 0))
    block = pl.BlockSpec((STAGE, width), lambda i: (i, 0))
    return pl.pallas_call(
        table_kernel,
        grid=(items // STAGE,),
        in_specs=[block, weight, pl.BlockSpec((1, width), lambda i: (0, 0)), weight, weight],
        out_specs=[block, block],
        out_shape=[jax.ShapeDtypeStruct((items, width), jnp.bfloat16)] * 2,
        compiler_params=pltpu.CompilerParams(dimension_semantics=("arbitrary",)),
        name="tables",
    )(items_table, message_weight, message_bias[None, :], neighbour_weight, self_weight)


def score_kernel(*refs):
    sums = refs[:4]
    count_ref, bias_ref, log_ref = refs[4:7]
    queries = refs[7 : 7 + 2 * SIDE]
    embed_ref, lse_ref, held, sems = refs[7 + 2 * SIDE :]
    f32 = jnp.float32
    rows = queries[0].shape[0]

    def copy(j, source):
        return pltpu.make_async_copy(source, held.at[pl.ds(j * rows, rows), :], sems.at[j])

    for j, source in enumerate(queries):
        copy(j, source).start()
    quarter = embed_ref.shape[0] // 4
    for q in range(4):
        at = slice(q * quarter, (q + 1) * quarter)
        hidden = jnp.maximum(sums[q][...] / count_ref[at, :] + bias_ref[...], 0.0)
        scale_inv = lax.rsqrt(jnp.mean(hidden * hidden, axis=-1, keepdims=True) + 0.25)
        embed_ref[at, :] = (hidden * scale_inv).astype(jnp.bfloat16)

    def block(j, _):
        copy(j, queries[0]).wait()

        def pair(i, _):
            first = j * rows + i * 2 * SCORED
            for u in range(2):
                at = pl.multiple_of(first + u * SCORED, SCORED)
                scores = lax.dot_general(
                    embed_ref[...], held[pl.ds(at, SCORED), :], (((1,), (1,)), ((), ())), preferred_element_type=f32
                )
                scores = 0.25 * scores - log_ref[...]
                peak = jnp.max(scores, axis=0, keepdims=True)
                total = jnp.sum(jnp.exp(scores - peak), axis=0, keepdims=True)
                lse_ref[pl.ds(at // SCORED, 1), :] = peak + jnp.log(total)
            return 0

        return lax.fori_loop(0, rows // (2 * SCORED), pair, 0)

    lax.fori_loop(0, len(queries), block, 0)


def scored(sums, count, bias, log_count, queries):
    negatives = count.shape[0]
    rows, width = queries[0].shape
    total = rows * len(queries)
    in_vmem = pl.BlockSpec(memory_space=pltpu.VMEM)
    return pl.pallas_call(
        score_kernel,
        in_specs=[in_vmem] * 7 + [pl.BlockSpec(memory_space=pl.ANY)] * len(queries),
        out_specs=[in_vmem] * 2,
        out_shape=[
            jax.ShapeDtypeStruct((negatives, width), jnp.bfloat16),
            jax.ShapeDtypeStruct((total // SCORED, SCORED), jnp.float32),
        ],
        scratch_shapes=[
            pltpu.VMEM((total, width), jnp.bfloat16),
            pltpu.SemaphoreType.DMA((len(queries),)),
        ],
        name="score",
    )(*sums, count[:, None], bias[None, :], log_count[:, None], *queries)


def per_device(
    items_table,
    fetch_rows,
    neighbour_slots,
    neighbour_count,
    self_slot,
    negative_count,
    message_weight,
    message_bias,
    self_weight,
    neighbour_weight,
    output_bias,
    queries,
):
    f32 = jnp.float32
    negatives = neighbour_count.shape[0]
    parts = lax.axis_size("neg")
    groups = lax.axis_size("qry")
    query_blocks = all_queries(queries)

    keys = composed_keys(neighbour_slots, self_slot, neighbour_count, fetch_rows).reshape(-1)
    bounds = jnp.array([min((p + 1 - 8) << 28, DEAD) for p in range(parts)], jnp.int32)
    ends = jnp.sum((keys[None, :] < bounds[:, None]).astype(jnp.int32), axis=1)
    lines = jnp.concatenate([lax.sort(keys, is_stable=False), ends, jnp.zeros((184 * LANES - keys.size - parts,), jnp.int32)])
    lists = from_everyone(lines.reshape(184, LANES), "neg")

    message_part, self_part = tables(items_table, message_weight, message_bias, neighbour_weight, self_weight)

    place = lax.axis_index("neg")
    part = jnp.stack([place // SIDE, place % SIDE]).astype(jnp.int32)
    outs = owner_sums(part, lists[:, keys.size // LANES, :parts], lists, message_part, self_part, negatives)
    sums = [q[0] for q in scattered_sums(outs)]

    own_count = lax.dynamic_slice(negative_count, (lax.axis_index("qry") * negatives,), (negatives,))
    log_count = jnp.log(own_count.astype(f32))
    negative_embed, part_lse = scored(sums, neighbour_count.astype(f32), output_bias, log_count, query_blocks)
    here = lax.axis_index("qry")
    z, core = here // 2, here % 2
    group = jnp.arange(groups)
    source = ((z - group // 2) % SIDE) + SIDE * ((group % 2) ^ core)
    picked = source[:, None] == group[None, :]
    blocks = part_lse.reshape(groups, -1)
    blocks = jnp.sum(jnp.where(picked[:, :, None], blocks[None], 0.0), axis=1)
    shared = jnp.broadcast_to(blocks[None], (parts, groups, queries.shape[0]))
    parts_lse = lax.all_to_all(
        shared.reshape(parts * groups, -1), ("neg", "qry"), split_axis=0, concat_axis=0, tiled=True
    )
    top = jnp.max(parts_lse, axis=0)
    query_lse = top + jnp.log(jnp.sum(jnp.exp(parts_lse - top[None, :]), axis=0))
    return (negative_embed, query_lse - math.log(negatives * parts * groups))


def solution(mesh):
    in_specs = (
        P("neg", None),
        P(("neg", "qry"), None),
        P(("neg", "qry"), None),
        P(("neg", "qry")),
        P(("neg", "qry")),
        P("neg"),
        P(),
        P(),
        P(),
        P(),
        P(),
        P("qry", None),
    )
    out_specs = (P(("neg", "qry"), None), P("qry"))

    return jax.shard_map(per_device, mesh=mesh, in_specs=in_specs, out_specs=out_specs, check_vma=False)
```

```python
import math

import jax
import jax.numpy as jnp
from jax import lax
from jax.experimental import pallas as pl
from jax.experimental.pallas import tpu as pltpu
from jax.sharding import PartitionSpec as P


LANES = 128
DEAD = 2**31 - 1
CHUNK = 128
STRIDE = 132
BLOCK = 10
STAGE = 1024
DEEP = 4
LINES = 176
COUNTS = 165
SIDE = 4
SCORED = 256
LOG2E = 1.4426950408889634
MESSAGES = 2 * SIDE


def compose_kernel(slots_ref, self_ref, count_ref, fetch_ref, keys_ref):
    neighbours, negatives = slots_ref.shape
    parts, per_part = fetch_ref.shape
    per_line = per_part // LANES
    half = parts // 2
    packed = fetch_ref[:half, :] | (fetch_ref[half:, :] << 13)
    lines = [
        jnp.broadcast_to(packed[p : p + 1, j * LANES : (j + 1) * LANES], (8, LANES))
        for p in range(half)
        for j in range(per_line)
    ]

    def located(slot):
        hi = slot >> 7
        lo = slot & 127
        upper = hi >= len(lines)
        folded = jnp.where(upper, hi - len(lines), hi)
        found = jnp.zeros_like(slot)
        for h, line in enumerate(lines):
            at = jnp.take_along_axis(line, lo, axis=1, mode="promise_in_bounds")
            found = jnp.where(folded == h, at, found)
        row = jnp.where(upper, found >> 13, found & 8191)
        return ((((hi * 205) >> 10) - 8) << 28) | row

    sublane = lax.broadcasted_iota(jnp.int32, (8, LANES), 0)
    lane = lax.broadcasted_iota(jnp.int32, (8, LANES), 1)
    for j in range(negatives // LANES):
        cols = slice(j * LANES, (j + 1) * LANES)
        count = jnp.broadcast_to(count_ref[:, cols], (8, LANES))
        for i in range(neighbours // 8):
            key = located(slots_ref[8 * i : 8 * (i + 1), cols]) | ((lane + j * LANES) << 19)
            first = (j * (neighbours // 8) + i) * 8
            keys_ref[first : first + 8, :] = jnp.where(sublane + 8 * i < count, key, DEAD)

    def tile_of(ref):
        tiles = [ref[:, j * LANES : (j + 1) * LANES] for j in range(negatives // LANES)]
        return jnp.concatenate(tiles + [jnp.zeros((8 - len(tiles), LANES), jnp.int32)], axis=0)

    own = located(tile_of(self_ref)) | ((sublane * LANES + lane) << 19)
    own = own | ((tile_of(count_ref) - 20) << 14) | (1 << 13)
    keys_ref[neighbours * negatives // LANES :, :] = own[: negatives // LANES]


def owner_kernel(part_ref, ends_ref, lists_ref, message_hbm, self_hbm, *refs):
    outs = refs[: 2 * MESSAGES]
    table, stage, pick, rows, acc, raw, weights, offsets, places, ready, sems, place_sem, out_sems = refs[2 * MESSAGES :]
    items = message_hbm.shape[0]
    width = message_hbm.shape[1]
    tiles = width // LANES
    per_table = items // STAGE
    step = pl.program_id(0)
    devices = pl.num_programs(0)
    part = part_ref[0] * SIDE + part_ref[1]
    negatives = pick.shape[0]
    quarter = negatives // 4

    def asker(i):
        x = (part_ref[0] + i // SIDE) % SIDE
        y = (part_ref[1] + i % SIDE) % SIDE
        return x * SIDE + y

    def range_of(r):
        return jnp.where(part == 0, 0, ends_ref[r, jnp.maximum(part - 1, 0)]), ends_ref[r, part]

    def place_copy():
        return pltpu.make_async_copy(offsets, places, place_sem)

    def place(r, base):
        for c in range(BLOCK):
            raw[c : c + 1, :] = lists_ref[r, pl.ds(base + c, 1), :]
        for half in range(2):
            at = slice(8 * half, 8 * half + 8)
            lines = raw[at, :]
            offsets[at, :] = (lines & 16383) * tiles
            v = (lines >> 16) & (negatives - 1)
            count = jnp.zeros_like(v)
            for q in range(negatives // LANES):
                counts = jnp.broadcast_to(lists_ref[r, COUNTS + q : COUNTS + q + 1, :], v.shape)
                found = jnp.take_along_axis(counts, v & (LANES - 1), axis=1, mode="promise_in_bounds")
                count = jnp.where(v >> 7 == q, found, count)
            weights[at, :] = jnp.where((lines & 8192) != 0, count, 1).astype(jnp.float32)
        place_copy().start()

    def stage_copy(c):
        source = message_hbm if c < per_table else self_hbm
        return pltpu.make_async_copy(
            source.at[pl.ds((c % per_table) * STAGE, STAGE), :], stage.at[c % DEEP], sems.at[c % DEEP]
        )

    def out_copy(slot, q, array, at):
        return pltpu.make_async_copy(
            ready.at[slot, pl.ds(q * quarter, quarter), :], array.at[at], out_sems.at[slot, q]
        )

    def wait_out(slot):
        for q in range(4):
            out_copy(slot, q, outs[0], 0).wait()

    @pl.when(step == 0)
    def _():
        for c in range(DEEP):
            stage_copy(c).start()
        raw[...] = jnp.zeros_like(raw)
        place(asker(0), range_of(asker(0))[0] >> 7)
        rows[...] = jnp.zeros_like(rows)
        for c in range(2 * per_table):
            stage_copy(c).wait()

            def spread(i, _, c=c):
                for u in range(4):
                    at = pl.multiple_of(i * 64 + u * 16, 16)
                    block = stage[c % DEEP, pl.ds(at, 16), :].astype(jnp.float32)
                    for half in range(2):
                        for j in range(tiles):
                            first = (c * STAGE + at + half * 8) * tiles + j
                            table[pl.ds(first, 8, stride=tiles), :] = block[
                                half * 8 : half * 8 + 8, j * LANES : (j + 1) * LANES
                            ]
                return 0

            lax.fori_loop(0, STAGE // 64, spread, 0)
            if c + DEEP < 2 * per_table:
                stage_copy(c + DEEP).start()

    a = asker(step)
    start, end = range_of(a)
    row_first = start >> 7
    row_last = (end + 127) >> 7

    def picked(r, line, weight):
        v = lax.broadcasted_iota(jnp.int32, (negatives, LANES), 0)
        at = r * LANES + lax.broadcasted_iota(jnp.int32, (1, LANES), 1)
        who = jnp.where((at >= start) & (at < end), line >> 16, -1)
        return jnp.where(v == who, weight, 0.0).astype(jnp.bfloat16)

    def gather(base):
        place_copy().wait()
        for c in range(BLOCK):
            r = base + c

            @pl.when(r < row_last)
            def _(c=c, r=r):
                pick[:, c * LANES : (c + 1) * LANES] = picked(r, raw[c : c + 1, :], weights[c : c + 1, :])
                for e in range(CHUNK):
                    at = pl.multiple_of(places[c, e], tiles)
                    rows[c, pl.ds(e, tiles, stride=STRIDE), :] = table[pl.ds(at, tiles), :]

            @pl.when(r >= row_last)
            def _(c=c):
                pick[:, c * LANES : (c + 1) * LANES] = jnp.zeros((negatives, LANES), jnp.bfloat16)

    def gather_more(base):
        place_copy().wait()

        def chunk(c, _):
            cols = pl.ds(pl.multiple_of(c * LANES, LANES), LANES)
            live = base + c < row_last
            one = pl.ds(c, 1)
            pick[:, cols] = jnp.where(live, picked(base + c, raw[one, :], weights[one, :]), 0).astype(jnp.bfloat16)

            def entry(e, _):
                at = pl.multiple_of(places[c, e], tiles)
                rows[c, pl.ds(e, tiles, stride=STRIDE), :] = table[pl.ds(at, tiles), :]
                return 0

            return lax.fori_loop(0, CHUNK, entry, 0)

        lax.fori_loop(0, BLOCK, chunk, 0)

    def summed():
        gathered = jnp.concatenate(
            [
                jnp.concatenate(
                    [rows[c, j * STRIDE : j * STRIDE + CHUNK, :].astype(jnp.bfloat16) for j in range(tiles)],
                    axis=1,
                )
                for c in range(BLOCK)
            ],
            axis=0,
        )
        return jnp.dot(pick[...], gathered, preferred_element_type=jnp.float32)

    gather(row_first)
    blocks = (row_last - row_first + BLOCK - 1) // BLOCK

    @pl.when((blocks <= 1) & (step + 1 < devices))
    def _():
        following = asker(step + 1)
        place(following, range_of(following)[0] >> 7)

    acc[...] = summed()

    @pl.when(blocks > 1)
    def _():
        def more(i, _):
            place(a, row_first + i * BLOCK)
            gather_more(row_first + i * BLOCK)
            acc[...] += summed()
            return 0

        lax.fori_loop(1, blocks, more, 0)

        @pl.when(step + 1 < devices)
        def _():
            following = asker(step + 1)
            place(following, range_of(following)[0] >> 7)

    slot = step % 2

    @pl.when(step >= 2)
    def _():
        wait_out(slot)

    ready[slot] = acc[...].astype(jnp.bfloat16)
    dx = step // SIDE
    dy = step % SIDE
    for d in range(SIDE):

        @pl.when(dx == d)
        def _(d=d):
            for h in range(2):
                out_copy(slot, h, outs[2 * d + h], dy).start()

        @pl.when(dy == d)
        def _(d=d):
            for h in range(2):
                out_copy(slot, 2 + h, outs[MESSAGES + 2 * d + h], dx).start()

    @pl.when(step + 1 == devices)
    def _():
        wait_out(slot)
        wait_out(1 - slot)


def from_everyone(x, axis):
    devices = lax.axis_size(axis)
    return lax.all_to_all(jnp.broadcast_to(x[None], (devices, *x.shape)), axis, 0, 0, tiled=True)


def composed_keys(neighbour_slots, self_slot, neighbour_count, fetch_rows):
    negatives, neighbours = neighbour_slots.shape
    folded = negatives // LANES
    return pl.pallas_call(
        compose_kernel,
        out_shape=jax.ShapeDtypeStruct(((neighbours + 1) * folded, LANES), jnp.int32),
        name="compose",
    )(
        neighbour_slots.T,
        self_slot[None, :],
        neighbour_count[None, :],
        fetch_rows,
    )


def owner_sums(part, ends, lists, message_part, self_part, negatives):
    devices, _, _ = lists.shape
    items, width = message_part.shape
    tiles = width // LANES
    quarter = [jax.ShapeDtypeStruct((SIDE, negatives // 4, width), jnp.bfloat16)]
    return pl.pallas_call(
        owner_kernel,
        grid=(devices,),
        in_specs=[
            pl.BlockSpec(memory_space=pltpu.SMEM),
            pl.BlockSpec(memory_space=pltpu.SMEM),
            pl.BlockSpec(memory_space=pltpu.VMEM),
            pl.BlockSpec(memory_space=pl.ANY),
            pl.BlockSpec(memory_space=pl.ANY),
        ],
        out_specs=[pl.BlockSpec(memory_space=pl.ANY)] * (2 * MESSAGES),
        out_shape=quarter * (2 * MESSAGES),
        scratch_shapes=[
            pltpu.VMEM((2 * items * tiles, LANES), jnp.float32),
            pltpu.VMEM((DEEP, STAGE, width), jnp.bfloat16),
            pltpu.VMEM((negatives, BLOCK * CHUNK), jnp.bfloat16),
            pltpu.VMEM((BLOCK, tiles * STRIDE, LANES), jnp.float32),
            pltpu.VMEM((negatives, width), jnp.float32),
            pltpu.VMEM((16, LANES), jnp.int32),
            pltpu.VMEM((16, LANES), jnp.float32),
            pltpu.VMEM((16, LANES), jnp.int32),
            pltpu.SMEM((16, LANES), jnp.int32),
            pltpu.VMEM((2, negatives, width), jnp.bfloat16),
            pltpu.SemaphoreType.DMA((DEEP,)),
            pltpu.SemaphoreType.DMA,
            pltpu.SemaphoreType.DMA((2, 4)),
        ],
        compiler_params=pltpu.CompilerParams(
            dimension_semantics=("arbitrary",), vmem_limit_bytes=60 * 2**20
        ),
        name="owner",
    )(part, ends, lists, message_part, self_part)


def moved(x, along, by):
    def place(i):
        x_at, y_at = divmod(i, SIDE)
        if along == "x":
            return (x_at + by) % SIDE * SIDE + y_at
        return x_at * SIDE + (y_at + by) % SIDE

    return lax.ppermute(x, "neg", [(i, place(i)) for i in range(SIDE * SIDE)])


def joined(*parts):
    return sum(p.astype(jnp.float32) for p in parts)


def ring_sums(parts, along):
    far_up = moved(parts[2][0], along, 1)
    far_down = moved(parts[2][1], along, -1)
    near_up = moved(parts[1][1], along, 1)
    near_down = moved(parts[3][0], along, -1)
    sent_up = moved(joined(parts[1][0], far_up).astype(jnp.bfloat16), along, 1)
    sent_down = moved(joined(parts[3][1], far_down).astype(jnp.bfloat16), along, -1)
    return joined(parts[0][0], sent_up, near_down), joined(parts[0][1], near_up, sent_down)


def joint_sums(own_first, own_second, up, down, next_up, next_down, along):
    half = up.shape[0] // 2
    came_up = moved(up, along, 1)
    came_down = moved(down, along, -1)
    sent_up = moved(joined(next_up, came_up[:half]).astype(jnp.bfloat16), along, 1)
    sent_down = moved(joined(next_down, came_down[:half]).astype(jnp.bfloat16), along, -1)
    return joined(own_first, sent_up, came_down[half:]), joined(own_second, came_up[half:], sent_down)


def scattered_sums(outs):
    result = []
    for at, order in ((0, "xy"), (MESSAGES, "yx")):
        parts = [outs[at + 2 * d : at + 2 * d + 2] for d in range(SIDE)]
        first, second = ring_sums(parts, order[0])
        low_first, low_second = first.astype(jnp.bfloat16), second.astype(jnp.bfloat16)
        up = jnp.concatenate([low_first[2:3], low_second[1:2]], axis=0)
        down = jnp.concatenate([low_second[2:3], low_first[3:4]], axis=0)
        result += joint_sums(first[0:1], second[0:1], up, down, low_first[1:2], low_second[3:4], order[1])
    return result


def turned(x, deep, other):
    def place(i):
        z, core = divmod(i, 2)
        return (z + deep) % SIDE * 2 + (1 - core if other else core)

    return lax.ppermute(x, "qry", [(i, place(i)) for i in range(2 * SIDE)])


def all_queries(queries):
    up = turned(queries, 1, False)
    down = turned(queries, -1, False)
    other = turned(queries, 0, True)
    far = turned(up, 1, False)
    other_up = turned(up, 0, True)
    other_down = turned(down, 0, True)
    other_far = turned(far, 0, True)
    return [queries, up, far, down, other, other_up, other_far, other_down]


def table_kernel(items_ref, message_ref, bias_ref, neighbour_ref, self_ref, message_out, self_out):
    f32 = jnp.float32
    items = items_ref[...]
    message = jnp.dot(items, message_ref[...], preferred_element_type=f32) + bias_ref[...]
    message = jnp.maximum(message, 0.0).astype(jnp.bfloat16)
    message_out[...] = jnp.dot(message, neighbour_ref[...], preferred_element_type=f32).astype(jnp.bfloat16)
    self_out[...] = jnp.dot(items, self_ref[...], preferred_element_type=f32).astype(jnp.bfloat16)


def tables(items_table, message_weight, message_bias, neighbour_weight, self_weight):
    items, width = items_table.shape
    weight = pl.BlockSpec((width, width), lambda i: (0, 0))
    block = pl.BlockSpec((STAGE, width), lambda i: (i, 0))
    return pl.pallas_call(
        table_kernel,
        grid=(items // STAGE,),
        in_specs=[block, weight, pl.BlockSpec((1, width), lambda i: (0, 0)), weight, weight],
        out_specs=[block, block],
        out_shape=[jax.ShapeDtypeStruct((items, width), jnp.bfloat16)] * 2,
        compiler_params=pltpu.CompilerParams(dimension_semantics=("arbitrary",)),
        name="tables",
    )(items_table, message_weight, message_bias[None, :], neighbour_weight, self_weight)


def score_kernel(*refs):
    sums = refs[:4]
    count_ref, bias_ref, log_ref = refs[4:7]
    queries = refs[7 : 7 + 2 * SIDE]
    embed_ref, lse_ref, held, even, odd, logs, sems = refs[7 + 2 * SIDE :]
    f32 = jnp.float32
    rows = queries[0].shape[0]
    blocks = len(queries) * rows // SCORED
    per_query = rows // SCORED

    def copy(j, source):
        return pltpu.make_async_copy(source, held.at[pl.ds(j * rows, rows), :], sems.at[j])

    for j, source in enumerate(queries):
        copy(j, source).start()
    negatives, width = embed_ref.shape

    def columns(row):
        return jnp.broadcast_to(row, (LANES, negatives)).T

    logs[...] = columns(jnp.log(log_ref[...].astype(f32)) * LOG2E)
    counts = columns(count_ref[...].astype(f32))
    quarter = negatives // 4
    for q in range(4):
        at = slice(q * quarter, (q + 1) * quarter)
        count = jnp.concatenate([counts[at, :]] * (width // LANES), axis=1)
        hidden = jnp.maximum(sums[q][...] / count + bias_ref[...], 0.0)
        scale_inv = lax.rsqrt(jnp.mean(hidden * hidden, axis=-1, keepdims=True) + 0.25)
        embed_ref[at, :] = (hidden * scale_inv).astype(jnp.bfloat16)

    def products(i):
        block = held[pl.ds(pl.multiple_of(i * SCORED, SCORED), SCORED), :]
        return lax.dot_general(embed_ref[...], block, (((1,), (1,)), ((), ())), preferred_element_type=f32)

    def reduced(ref, i):
        found = []
        for j in range(SCORED // LANES):
            lane = slice(j * LANES, (j + 1) * LANES)
            scores = ref[:, lane] * (0.25 * LOG2E) - logs[...]
            peak = jnp.max(scores, axis=0, keepdims=True)
            total = jnp.sum(jnp.exp2(scores - peak), axis=0, keepdims=True)
            found.append((peak + jnp.log2(total)) * (1.0 / LOG2E))
        lse_ref[pl.ds(i, 1), :] = jnp.concatenate(found, axis=1)

    copy(0, queries[0]).wait()
    even[...] = products(0)

    def pair(i, _):
        following = jnp.minimum(2 * i + 2, blocks - 1)

        @pl.when((following % per_query == 0) & (2 * i + 2 < blocks))
        def _():
            copy(following // per_query, queries[0]).wait()

        odd[...] = products(2 * i + 1)
        reduced(even, 2 * i)
        even[...] = products(following)
        reduced(odd, 2 * i + 1)
        return 0

    lax.fori_loop(0, blocks // 2, pair, 0)


def scored(sums, count, bias, own_count, queries):
    negatives = count.shape[0]
    rows, width = queries[0].shape
    total = rows * len(queries)
    in_vmem = pl.BlockSpec(memory_space=pltpu.VMEM)
    return pl.pallas_call(
        score_kernel,
        in_specs=[in_vmem] * 7 + [pl.BlockSpec(memory_space=pl.ANY)] * len(queries),
        out_specs=[in_vmem] * 2,
        out_shape=[
            jax.ShapeDtypeStruct((negatives, width), jnp.bfloat16),
            jax.ShapeDtypeStruct((total // SCORED, SCORED), jnp.float32),
        ],
        scratch_shapes=[
            pltpu.VMEM((total, width), jnp.bfloat16),
            pltpu.VMEM((negatives, SCORED), jnp.float32),
            pltpu.VMEM((negatives, SCORED), jnp.float32),
            pltpu.VMEM((negatives, LANES), jnp.float32),
            pltpu.SemaphoreType.DMA((len(queries),)),
        ],
        name="score",
    )(*sums, count[None, :], bias[None, :], own_count[None, :], *queries)


def per_device(
    items_table,
    fetch_rows,
    neighbour_slots,
    neighbour_count,
    self_slot,
    negative_count,
    message_weight,
    message_bias,
    self_weight,
    neighbour_weight,
    output_bias,
    queries,
):
    negatives = neighbour_count.shape[0]
    parts = lax.axis_size("neg")
    groups = lax.axis_size("qry")
    query_blocks = all_queries(queries)

    keys = composed_keys(neighbour_slots, self_slot, neighbour_count, fetch_rows).reshape(-1)
    bounds = jnp.array([min((p + 1 - 8) << 28, DEAD) for p in range(parts)], jnp.int32)
    ends = jnp.sum((keys[None, :] < bounds[:, None]).astype(jnp.int32), axis=1)
    ordered = lax.sort(keys, is_stable=False)
    ordered = (((ordered >> 19) & (negatives - 1)) << 16) | (ordered & 16383)
    tail = jnp.zeros((LINES * LANES - keys.size - LANES - negatives,), jnp.int32)
    lines = jnp.concatenate([ordered, jnp.pad(ends, (0, LANES - parts)), neighbour_count, tail])
    lists = from_everyone(lines.reshape(LINES, LANES), "neg")

    message_part, self_part = tables(items_table, message_weight, message_bias, neighbour_weight, self_weight)

    own_count = lax.dynamic_slice(negative_count, (lax.axis_index("qry") * negatives,), (negatives,))
    place = lax.axis_index("neg")
    part = jnp.stack([place // SIDE, place % SIDE]).astype(jnp.int32)
    outs = owner_sums(part, lists[:, keys.size // LANES, :parts], lists, message_part, self_part, negatives)
    sums = [q[0] for q in scattered_sums(outs)]

    negative_embed, part_lse = scored(sums, neighbour_count, output_bias, own_count, query_blocks)
    here = lax.axis_index("qry")
    z, core = here // 2, here % 2
    group = jnp.arange(groups)
    source = ((z - group // 2) % SIDE) + SIDE * ((group % 2) ^ core)
    picked = source[:, None] == group[None, :]
    blocks = part_lse.reshape(groups, -1)
    blocks = jnp.sum(jnp.where(picked[:, :, None], blocks[None], 0.0), axis=1)
    shared = jnp.broadcast_to(blocks[None], (parts, groups, queries.shape[0]))
    parts_lse = lax.all_to_all(
        shared.reshape(parts * groups, -1), ("neg", "qry"), split_axis=0, concat_axis=0, tiled=True
    )
    top = jnp.max(parts_lse, axis=0)
    query_lse = top + jnp.log(jnp.sum(jnp.exp(parts_lse - top[None, :]), axis=0))
    return (negative_embed, query_lse - math.log(negatives * parts * groups))


def solution(mesh):
    in_specs = (
        P("neg", None),
        P(("neg", "qry"), None),
        P(("neg", "qry"), None),
        P(("neg", "qry")),
        P(("neg", "qry")),
        P("neg"),
        P(),
        P(),
        P(),
        P(),
        P(),
        P("qry", None),
    )
    out_specs = (P(("neg", "qry"), None), P("qry"))

    return jax.shard_map(per_device, mesh=mesh, in_specs=in_specs, out_specs=out_specs, check_vma=False)
```

```python
import functools
import math

import jax
import jax.numpy as jnp
from jax import lax
from jax.experimental import pallas as pl
from jax.experimental.pallas import tpu as pltpu
from jax.sharding import PartitionSpec as P


LANES = 128
DEAD = 2**31 - 1
CHUNK = 128
STRIDE = 132
BLOCK = 10
STAGE = 1024
DEEP = 4
LINES = 176
COUNTS = 165
SIDE = 4
SCORED = 256
LOG2E = 1.4426950408889634
MESSAGES = 2 * SIDE


def compose_kernel(slots_ref, self_ref, count_ref, fetch_ref, keys_ref):
    neighbours, negatives = slots_ref.shape
    parts, per_part = fetch_ref.shape
    per_line = per_part // LANES
    half = parts // 2
    packed = fetch_ref[:half, :] | (fetch_ref[half:, :] << 13)
    lines = [
        jnp.broadcast_to(packed[p : p + 1, j * LANES : (j + 1) * LANES], (8, LANES))
        for p in range(half)
        for j in range(per_line)
    ]

    def located(slot):
        hi = slot >> 7
        lo = slot & 127
        upper = hi >= len(lines)
        folded = jnp.where(upper, hi - len(lines), hi)
        found = jnp.zeros_like(slot)
        for h, line in enumerate(lines):
            at = jnp.take_along_axis(line, lo, axis=1, mode="promise_in_bounds")
            found = jnp.where(folded == h, at, found)
        row = jnp.where(upper, found >> 13, found & 8191)
        return ((((hi * 205) >> 10) - 8) << 28) | row

    sublane = lax.broadcasted_iota(jnp.int32, (8, LANES), 0)
    lane = lax.broadcasted_iota(jnp.int32, (8, LANES), 1)
    for j in range(negatives // LANES):
        cols = slice(j * LANES, (j + 1) * LANES)
        count = jnp.broadcast_to(count_ref[:, cols], (8, LANES))
        for i in range(neighbours // 8):
            key = located(slots_ref[8 * i : 8 * (i + 1), cols]) | ((lane + j * LANES) << 19)
            first = (j * (neighbours // 8) + i) * 8
            keys_ref[first : first + 8, :] = jnp.where(sublane + 8 * i < count, key, DEAD)

    def tile_of(ref):
        tiles = [ref[:, j * LANES : (j + 1) * LANES] for j in range(negatives // LANES)]
        return jnp.concatenate(tiles + [jnp.zeros((8 - len(tiles), LANES), jnp.int32)], axis=0)

    own = located(tile_of(self_ref)) | ((sublane * LANES + lane) << 19)
    own = own | ((tile_of(count_ref) - 20) << 14) | (1 << 13)
    keys_ref[neighbours * negatives // LANES :, :] = own[: negatives // LANES]


def owner_kernel(part_ref, ends_ref, lists_ref, message_hbm, self_hbm, *refs):
    outs = refs[: 2 * MESSAGES]
    table, stage, pick, rows, acc, raw, weights, offsets, places, ready, sems, place_sem, out_sems = refs[2 * MESSAGES :]
    items = message_hbm.shape[0]
    width = message_hbm.shape[1]
    tiles = width // LANES
    per_table = items // STAGE
    step = pl.program_id(0)
    devices = pl.num_programs(0)
    part = part_ref[0] * SIDE + part_ref[1]
    negatives = pick.shape[0]
    quarter = negatives // 4

    def asker(i):
        x = (part_ref[0] + i // SIDE) % SIDE
        y = (part_ref[1] + i % SIDE) % SIDE
        return x * SIDE + y

    def range_of(r):
        return jnp.where(part == 0, 0, ends_ref[r, jnp.maximum(part - 1, 0)]), ends_ref[r, part]

    def place_copy():
        return pltpu.make_async_copy(offsets, places, place_sem)

    def place(r, base):
        for c in range(BLOCK):
            raw[c : c + 1, :] = lists_ref[r, pl.ds(base + c, 1), :]
        for half in range(2):
            at = slice(8 * half, 8 * half + 8)
            lines = raw[at, :]
            offsets[at, :] = (lines & 16383) * tiles
            v = (lines >> 16) & (negatives - 1)
            count = jnp.zeros_like(v)
            for q in range(negatives // LANES):
                counts = jnp.broadcast_to(lists_ref[r, COUNTS + q : COUNTS + q + 1, :], v.shape)
                found = jnp.take_along_axis(counts, v & (LANES - 1), axis=1, mode="promise_in_bounds")
                count = jnp.where(v >> 7 == q, found, count)
            weights[at, :] = jnp.where((lines & 8192) != 0, count, 1).astype(jnp.float32)
        place_copy().start()

    def stage_copy(c):
        source = message_hbm if c < per_table else self_hbm
        return pltpu.make_async_copy(
            source.at[pl.ds((c % per_table) * STAGE, STAGE), :], stage.at[c % DEEP], sems.at[c % DEEP]
        )

    def out_copy(slot, q, array, at):
        return pltpu.make_async_copy(
            ready.at[slot, pl.ds(q * quarter, quarter), :], array.at[at], out_sems.at[slot, q]
        )

    def wait_out(slot):
        for q in range(4):
            out_copy(slot, q, outs[0], 0).wait()

    @pl.when(step == 0)
    def _():
        for c in range(DEEP):
            stage_copy(c).start()
        raw[...] = jnp.zeros_like(raw)
        place(asker(0), range_of(asker(0))[0] >> 7)
        rows[...] = jnp.zeros_like(rows)
        for c in range(2 * per_table):
            stage_copy(c).wait()

            def spread(i, _, c=c):
                for u in range(4):
                    at = pl.multiple_of(i * 64 + u * 16, 16)
                    block = stage[c % DEEP, pl.ds(at, 16), :].astype(jnp.float32)
                    for half in range(2):
                        for j in range(tiles):
                            first = (c * STAGE + at + half * 8) * tiles + j
                            table[pl.ds(first, 8, stride=tiles), :] = block[
                                half * 8 : half * 8 + 8, j * LANES : (j + 1) * LANES
                            ]
                return 0

            lax.fori_loop(0, STAGE // 64, spread, 0)
            if c + DEEP < 2 * per_table:
                stage_copy(c + DEEP).start()

    a = asker(step)
    start, end = range_of(a)
    row_first = start >> 7
    row_last = (end + 127) >> 7

    def picked(r, line, weight):
        v = lax.broadcasted_iota(jnp.int32, (negatives, LANES), 0)
        at = r * LANES + lax.broadcasted_iota(jnp.int32, (1, LANES), 1)
        who = jnp.where((at >= start) & (at < end), line >> 16, -1)
        return jnp.where(v == who, weight, 0.0).astype(jnp.bfloat16)

    def gather(base):
        place_copy().wait()
        for c in range(BLOCK):
            r = base + c

            @pl.when(r < row_last)
            def _(c=c, r=r):
                pick[:, c * LANES : (c + 1) * LANES] = picked(r, raw[c : c + 1, :], weights[c : c + 1, :])
                for e in range(CHUNK):
                    at = pl.multiple_of(places[c, e], tiles)
                    rows[c, pl.ds(e, tiles, stride=STRIDE), :] = table[pl.ds(at, tiles), :]

            @pl.when(r >= row_last)
            def _(c=c):
                pick[:, c * LANES : (c + 1) * LANES] = jnp.zeros((negatives, LANES), jnp.bfloat16)

    def gather_more(base):
        place_copy().wait()

        def chunk(c, _):
            cols = pl.ds(pl.multiple_of(c * LANES, LANES), LANES)
            live = base + c < row_last
            one = pl.ds(c, 1)
            pick[:, cols] = jnp.where(live, picked(base + c, raw[one, :], weights[one, :]), 0).astype(jnp.bfloat16)

            def entry(e, _):
                at = pl.multiple_of(places[c, e], tiles)
                rows[c, pl.ds(e, tiles, stride=STRIDE), :] = table[pl.ds(at, tiles), :]
                return 0

            return lax.fori_loop(0, CHUNK, entry, 0)

        lax.fori_loop(0, BLOCK, chunk, 0)

    def summed():
        gathered = jnp.concatenate(
            [
                jnp.concatenate(
                    [rows[c, j * STRIDE : j * STRIDE + CHUNK, :].astype(jnp.bfloat16) for j in range(tiles)],
                    axis=1,
                )
                for c in range(BLOCK)
            ],
            axis=0,
        )
        return jnp.dot(pick[...], gathered, preferred_element_type=jnp.float32)

    gather(row_first)
    blocks = (row_last - row_first + BLOCK - 1) // BLOCK

    @pl.when((blocks <= 1) & (step + 1 < devices))
    def _():
        following = asker(step + 1)
        place(following, range_of(following)[0] >> 7)

    acc[...] = summed()

    @pl.when(blocks > 1)
    def _():
        def more(i, _):
            place(a, row_first + i * BLOCK)
            gather_more(row_first + i * BLOCK)
            acc[...] += summed()
            return 0

        lax.fori_loop(1, blocks, more, 0)

        @pl.when(step + 1 < devices)
        def _():
            following = asker(step + 1)
            place(following, range_of(following)[0] >> 7)

    slot = step % 2

    @pl.when(step >= 2)
    def _():
        wait_out(slot)

    ready[slot] = acc[...].astype(jnp.bfloat16)
    dx = step // SIDE
    dy = step % SIDE
    for d in range(SIDE):

        @pl.when(dx == d)
        def _(d=d):
            for h in range(2):
                out_copy(slot, h, outs[2 * d + h], dy).start()

        @pl.when(dy == d)
        def _(d=d):
            for h in range(2):
                out_copy(slot, 2 + h, outs[MESSAGES + 2 * d + h], dx).start()

    @pl.when(step + 1 == devices)
    def _():
        wait_out(slot)
        wait_out(1 - slot)


def from_everyone(x, axis):
    devices = lax.axis_size(axis)
    return lax.all_to_all(jnp.broadcast_to(x[None], (devices, *x.shape)), axis, 0, 0, tiled=True)


def composed_keys(neighbour_slots, self_slot, neighbour_count, fetch_rows):
    negatives, neighbours = neighbour_slots.shape
    folded = negatives // LANES
    return pl.pallas_call(
        compose_kernel,
        out_shape=jax.ShapeDtypeStruct(((neighbours + 1) * folded, LANES), jnp.int32),
        name="compose",
    )(
        neighbour_slots.T,
        self_slot[None, :],
        neighbour_count[None, :],
        fetch_rows,
    )


def owner_sums(part, ends, lists, message_part, self_part, negatives):
    devices, _, _ = lists.shape
    items, width = message_part.shape
    tiles = width // LANES
    quarter = [jax.ShapeDtypeStruct((SIDE, negatives // 4, width), jnp.bfloat16)]
    return pl.pallas_call(
        owner_kernel,
        grid=(devices,),
        in_specs=[
            pl.BlockSpec(memory_space=pltpu.SMEM),
            pl.BlockSpec(memory_space=pltpu.SMEM),
            pl.BlockSpec(memory_space=pltpu.VMEM),
            pl.BlockSpec(memory_space=pl.ANY),
            pl.BlockSpec(memory_space=pl.ANY),
        ],
        out_specs=[pl.BlockSpec(memory_space=pl.ANY)] * (2 * MESSAGES),
        out_shape=quarter * (2 * MESSAGES),
        scratch_shapes=[
            pltpu.VMEM((2 * items * tiles, LANES), jnp.float32),
            pltpu.VMEM((DEEP, STAGE, width), jnp.bfloat16),
            pltpu.VMEM((negatives, BLOCK * CHUNK), jnp.bfloat16),
            pltpu.VMEM((BLOCK, tiles * STRIDE, LANES), jnp.float32),
            pltpu.VMEM((negatives, width), jnp.float32),
            pltpu.VMEM((16, LANES), jnp.int32),
            pltpu.VMEM((16, LANES), jnp.float32),
            pltpu.VMEM((16, LANES), jnp.int32),
            pltpu.SMEM((16, LANES), jnp.int32),
            pltpu.VMEM((2, negatives, width), jnp.bfloat16),
            pltpu.SemaphoreType.DMA((DEEP,)),
            pltpu.SemaphoreType.DMA,
            pltpu.SemaphoreType.DMA((2, 4)),
        ],
        compiler_params=pltpu.CompilerParams(
            dimension_semantics=("arbitrary",), vmem_limit_bytes=60 * 2**20
        ),
        name="owner",
    )(part, ends, lists, message_part, self_part)


def moved(x, along, by):
    def place(i):
        x_at, y_at = divmod(i, SIDE)
        if along == "x":
            return (x_at + by) % SIDE * SIDE + y_at
        return x_at * SIDE + (y_at + by) % SIDE

    return lax.ppermute(x, "neg", [(i, place(i)) for i in range(SIDE * SIDE)])


def joined(*parts):
    return sum(p.astype(jnp.float32) for p in parts)


def ring_sums(parts, along):
    far_up = moved(parts[2][0], along, 1)
    far_down = moved(parts[2][1], along, -1)
    near_up = moved(parts[1][1], along, 1)
    near_down = moved(parts[3][0], along, -1)
    sent_up = moved(joined(parts[1][0], far_up).astype(jnp.bfloat16), along, 1)
    sent_down = moved(joined(parts[3][1], far_down).astype(jnp.bfloat16), along, -1)
    return joined(parts[0][0], sent_up, near_down), joined(parts[0][1], near_up, sent_down)


def joint_sums(own_first, own_second, up, down, next_up, next_down, along):
    half = up.shape[0] // 2
    came_up = moved(up, along, 1)
    came_down = moved(down, along, -1)
    sent_up = moved(joined(next_up, came_up[:half]).astype(jnp.bfloat16), along, 1)
    sent_down = moved(joined(next_down, came_down[:half]).astype(jnp.bfloat16), along, -1)
    return joined(own_first, sent_up, came_down[half:]), joined(own_second, came_up[half:], sent_down)


def scattered_sums(outs):
    result = []
    for at, order in ((0, "xy"), (MESSAGES, "yx")):
        parts = [outs[at + 2 * d : at + 2 * d + 2] for d in range(SIDE)]
        first, second = ring_sums(parts, order[0])
        low_first, low_second = first.astype(jnp.bfloat16), second.astype(jnp.bfloat16)
        up = jnp.concatenate([low_first[2:3], low_second[1:2]], axis=0)
        down = jnp.concatenate([low_second[2:3], low_first[3:4]], axis=0)
        result += joint_sums(first[0:1], second[0:1], up, down, low_first[1:2], low_second[3:4], order[1])
    return result


def turned(x, deep, other):
    def place(i):
        z, core = divmod(i, 2)
        return (z + deep) % SIDE * 2 + (1 - core if other else core)

    return lax.ppermute(x, "qry", [(i, place(i)) for i in range(2 * SIDE)])


def all_queries(queries):
    up = turned(queries, 1, False)
    down = turned(queries, -1, False)
    other = turned(queries, 0, True)
    far = turned(up, 1, False)
    other_up = turned(up, 0, True)
    other_down = turned(down, 0, True)
    other_far = turned(far, 0, True)
    return [queries, up, far, down, other, other_up, other_far, other_down]


def table_kernel(items_ref, message_ref, bias_ref, neighbour_ref, self_ref, message_out, self_out):
    f32 = jnp.float32
    items = items_ref[...]
    message = jnp.dot(items, message_ref[...], preferred_element_type=f32) + bias_ref[...]
    message = jnp.maximum(message, 0.0).astype(jnp.bfloat16)
    message_out[...] = jnp.dot(message, neighbour_ref[...], preferred_element_type=f32).astype(jnp.bfloat16)
    self_out[...] = jnp.dot(items, self_ref[...], preferred_element_type=f32).astype(jnp.bfloat16)


def tables(items_table, message_weight, message_bias, neighbour_weight, self_weight):
    items, width = items_table.shape
    weight = pl.BlockSpec((width, width), lambda i: (0, 0))
    block = pl.BlockSpec((STAGE, width), lambda i: (i, 0))
    return pl.pallas_call(
        table_kernel,
        grid=(items // STAGE,),
        in_specs=[block, weight, pl.BlockSpec((1, width), lambda i: (0, 0)), weight, weight],
        out_specs=[block, block],
        out_shape=[jax.ShapeDtypeStruct((items, width), jnp.bfloat16)] * 2,
        compiler_params=pltpu.CompilerParams(dimension_semantics=("arbitrary",)),
        name="tables",
    )(items_table, message_weight, message_bias[None, :], neighbour_weight, self_weight)


def score_kernel(*refs, first, many):
    sums = refs[:2]
    place_ref, count_ref, bias_ref, log_ref, earlier_ref = refs[2:7]
    queries = refs[7 : 7 + many]
    embed_ref, lse_ref, held, even, odd, logs, sems = refs[7 + many :]
    f32 = jnp.float32
    rows = queries[0].shape[0]
    blocks = many * rows // SCORED
    per_query = rows // SCORED
    negatives, width = embed_ref.shape
    here = slice(first, first + negatives)

    def copy(j, source):
        return pltpu.make_async_copy(source, held.at[pl.ds(j * rows, rows), :], sems.at[j])

    for j, source in enumerate(queries):
        copy(j, source).start()

    def columns(row):
        return jnp.broadcast_to(row, (LANES, negatives)).T

    own = log_ref[pl.ds(place_ref[0], 1), :][:, here]
    logs[...] = columns(jnp.log(own.astype(f32)) * LOG2E)
    counts = columns(count_ref[:, here].astype(f32))
    half = negatives // 2
    for q in range(2):
        at = slice(q * half, (q + 1) * half)
        count = jnp.concatenate([counts[at, :]] * (width // LANES), axis=1)
        hidden = jnp.maximum(sums[q][...] / count + bias_ref[...], 0.0)
        scale_inv = lax.rsqrt(jnp.mean(hidden * hidden, axis=-1, keepdims=True) + 0.25)
        embed_ref[at, :] = (hidden * scale_inv).astype(jnp.bfloat16)

    def products(i):
        block = held[pl.ds(pl.multiple_of(i * SCORED, SCORED), SCORED), :]
        return lax.dot_general(embed_ref[...], block, (((1,), (1,)), ((), ())), preferred_element_type=f32)

    def reduced(ref, i):
        found = []
        for j in range(SCORED // LANES):
            lane = slice(j * LANES, (j + 1) * LANES)
            scores = ref[:, lane] * (0.25 * LOG2E) - logs[...]
            peak = jnp.max(scores, axis=0, keepdims=True)
            total = jnp.sum(jnp.exp2(scores - peak), axis=0, keepdims=True)
            found.append((peak + jnp.log2(total)) * (1.0 / LOG2E))
        found = jnp.concatenate(found, axis=1)
        if earlier_ref is not None:
            other = earlier_ref[pl.ds(i, 1), :]
            peak = jnp.maximum(found, other)
            found = peak + jnp.log(jnp.exp(found - peak) + jnp.exp(other - peak))
        lse_ref[pl.ds(i, 1), :] = found

    copy(0, queries[0]).wait()
    even[...] = products(0)

    def pair(i, _):
        following = jnp.minimum(2 * i + 2, blocks - 1)

        @pl.when((following % per_query == 0) & (2 * i + 2 < blocks))
        def _():
            copy(following // per_query, queries[0]).wait()

        odd[...] = products(2 * i + 1)
        reduced(even, 2 * i)
        even[...] = products(following)
        reduced(odd, 2 * i + 1)
        return 0

    lax.fori_loop(0, blocks // 2, pair, 0)


def scored(sums, first, place, count, bias, counts_all, earlier, queries):
    negatives = 2 * sums[0].shape[0]
    rows, width = queries[0].shape
    many = len(queries)
    total = rows * many
    in_vmem = pl.BlockSpec(memory_space=pltpu.VMEM)
    kernel = functools.partial(score_kernel, first=first, many=many)
    if earlier is None:
        body = kernel

        def kernel(*refs):
            return body(*refs[:6], None, *refs[6:])

    extra = [] if earlier is None else [earlier]
    return pl.pallas_call(
        kernel,
        in_specs=[in_vmem] * 2
        + [pl.BlockSpec(memory_space=pltpu.SMEM)]
        + [in_vmem] * (3 + len(extra))
        + [pl.BlockSpec(memory_space=pl.ANY)] * many,
        out_specs=[in_vmem] * 2,
        out_shape=[
            jax.ShapeDtypeStruct((negatives, width), jnp.bfloat16),
            jax.ShapeDtypeStruct((total // SCORED, SCORED), jnp.float32),
        ],
        scratch_shapes=[
            pltpu.VMEM((total, width), jnp.bfloat16),
            pltpu.VMEM((negatives, SCORED), jnp.float32),
            pltpu.VMEM((negatives, SCORED), jnp.float32),
            pltpu.VMEM((negatives, LANES), jnp.float32),
            pltpu.SemaphoreType.DMA((many,)),
        ],
        name="score",
    )(*sums, place, count, bias[None, :], counts_all, *extra, *queries)


def per_device(
    items_table,
    fetch_rows,
    neighbour_slots,
    neighbour_count,
    self_slot,
    negative_count,
    message_weight,
    message_bias,
    self_weight,
    neighbour_weight,
    output_bias,
    queries,
):
    negatives = neighbour_count.shape[0]
    parts = lax.axis_size("neg")
    groups = lax.axis_size("qry")
    query_blocks = all_queries(queries)

    keys = composed_keys(neighbour_slots, self_slot, neighbour_count, fetch_rows).reshape(-1)
    bounds = jnp.array([min((p + 1 - 8) << 28, DEAD) for p in range(parts)], jnp.int32)
    ends = jnp.sum((keys[None, :] < bounds[:, None]).astype(jnp.int32), axis=1)
    ordered = lax.sort(keys, is_stable=False)
    ordered = (((ordered >> 19) & (negatives - 1)) << 16) | (ordered & 16383)
    tail = jnp.zeros((LINES * LANES - keys.size - LANES - negatives,), jnp.int32)
    lines = jnp.concatenate([ordered, jnp.pad(ends, (0, LANES - parts)), neighbour_count, tail])
    lists = from_everyone(lines.reshape(LINES, LANES), "neg")

    message_part, self_part = tables(items_table, message_weight, message_bias, neighbour_weight, self_weight)

    place = lax.axis_index("neg")
    part = jnp.stack([place // SIDE, place % SIDE]).astype(jnp.int32)
    outs = owner_sums(part, lists[:, keys.size // LANES, :parts], lists, message_part, self_part, negatives)
    sums = [q[0] for q in scattered_sums(outs)]

    here = lax.axis_index("qry")
    whole = (here.reshape(1), neighbour_count[None, :], output_bias, negative_count.reshape(groups, negatives))
    early_embed, early_lse = scored(sums[:2], 0, *whole, None, query_blocks)
    late_embed, part_lse = scored(sums[2:], negatives // 2, *whole, early_lse, query_blocks)
    negative_embed = jnp.concatenate([early_embed, late_embed], axis=0)
    z, core = here // 2, here % 2
    group = jnp.arange(groups)
    source = ((z - group // 2) % SIDE) + SIDE * ((group % 2) ^ core)
    picked = source[:, None] == group[None, :]
    blocks = part_lse.reshape(groups, -1)
    blocks = jnp.sum(jnp.where(picked[:, :, None], blocks[None], 0.0), axis=1)
    shared = jnp.broadcast_to(blocks[None], (parts, groups, queries.shape[0]))
    parts_lse = lax.all_to_all(
        shared.reshape(parts * groups, -1), ("neg", "qry"), split_axis=0, concat_axis=0, tiled=True
    )
    top = jnp.max(parts_lse, axis=0)
    query_lse = top + jnp.log(jnp.sum(jnp.exp(parts_lse - top[None, :]), axis=0))
    return (negative_embed, query_lse - math.log(negatives * parts * groups))


def solution(mesh):
    in_specs = (
        P("neg", None),
        P(("neg", "qry"), None),
        P(("neg", "qry"), None),
        P(("neg", "qry")),
        P(("neg", "qry")),
        P("neg"),
        P(),
        P(),
        P(),
        P(),
        P(),
        P("qry", None),
    )
    out_specs = (P(("neg", "qry"), None), P("qry"))

    return jax.shard_map(per_device, mesh=mesh, in_specs=in_specs, out_specs=out_specs, check_vma=False)
```

```python
import math

import jax
import jax.numpy as jnp
from jax import lax
from jax.experimental import pallas as pl
from jax.experimental.pallas import tpu as pltpu
from jax.sharding import PartitionSpec as P


LANES = 128
DEAD = 2**31 - 1
CHUNK = 128
STRIDE = 132
BLOCK = 10
USUAL = 8
STAGE = 1024
DEEP = 4
LINES = 176
COUNTS = 165
SIDE = 4
SCORED = 512
LOG2E = 1.4426950408889634
MESSAGES = 2 * SIDE


def compose_kernel(slots_ref, self_ref, count_ref, fetch_ref, keys_ref, ends_ref):
    neighbours, negatives = slots_ref.shape
    parts, per_part = fetch_ref.shape
    per_line = per_part // LANES
    half = parts // 2
    packed = fetch_ref[:half, :] | (fetch_ref[half:, :] << 13)
    lines = [
        jnp.broadcast_to(packed[p : p + 1, j * LANES : (j + 1) * LANES], (8, LANES))
        for p in range(half)
        for j in range(per_line)
    ]

    def located(slot):
        hi = slot >> 7
        lo = slot & 127
        upper = hi >= len(lines)
        folded = jnp.where(upper, hi - len(lines), hi)
        found = jnp.zeros_like(slot)
        for h, line in enumerate(lines):
            at = jnp.take_along_axis(line, lo, axis=1, mode="promise_in_bounds")
            found = jnp.where(folded == h, at, found)
        row = jnp.where(upper, found >> 13, found & 8191)
        return ((((hi * 205) >> 10) - 8) << 28) | row

    sublane = lax.broadcasted_iota(jnp.int32, (8, LANES), 0)
    lane = lax.broadcasted_iota(jnp.int32, (8, LANES), 1)
    for j in range(negatives // LANES):
        cols = slice(j * LANES, (j + 1) * LANES)
        count = jnp.broadcast_to(count_ref[:, cols], (8, LANES))
        for i in range(neighbours // 8):
            key = located(slots_ref[8 * i : 8 * (i + 1), cols]) | ((lane + j * LANES) << 19)
            first = (j * (neighbours // 8) + i) * 8
            keys_ref[first : first + 8, :] = jnp.where(sublane + 8 * i < count, key, DEAD)

    def tile_of(ref):
        tiles = [ref[:, j * LANES : (j + 1) * LANES] for j in range(negatives // LANES)]
        return jnp.concatenate(tiles + [jnp.zeros((8 - len(tiles), LANES), jnp.int32)], axis=0)

    own = located(tile_of(self_ref)) | ((sublane * LANES + lane) << 19)
    own = own | ((tile_of(count_ref) - 20) << 14) | (1 << 13)
    keys_ref[neighbours * negatives // LANES :, :] = own[: negatives // LANES]

    keys = keys_ref[...]
    at = lax.broadcasted_iota(jnp.int32, (1, LANES), 1)
    ends = jnp.zeros((1, LANES), jnp.int32)
    for p in range(parts):
        below = jnp.sum((keys < min((p + 1 - 8) << 28, DEAD)).astype(jnp.int32), axis=0, keepdims=True)
        ends = jnp.where(at == p, jnp.sum(below, axis=1, keepdims=True), ends)
    ends_ref[...] = ends


def pack_kernel(keys_ref, ends_ref, count_ref, out_ref):
    entries = keys_ref.shape[0]
    negatives = count_ref.shape[1]
    keys = keys_ref[...]
    lines = (((keys >> 19) & (negatives - 1)) << 16) | (keys & 16383)
    count = [count_ref[:, q * LANES : (q + 1) * LANES] for q in range(negatives // LANES)]
    for p in range(out_ref.shape[0]):
        out_ref[p, :entries, :] = lines
        out_ref[p, entries : entries + 1, :] = ends_ref[...]
        for q, line in enumerate(count):
            out_ref[p, COUNTS + q : COUNTS + q + 1, :] = line
        out_ref[p, COUNTS + len(count) :, :] = jnp.zeros((LINES - COUNTS - len(count), LANES), jnp.int32)


def packed_lists(keys, ends, neighbour_count, devices):
    return pl.pallas_call(
        pack_kernel,
        out_shape=jax.ShapeDtypeStruct((devices, LINES, LANES), jnp.int32),
        name="pack",
    )(keys, ends, neighbour_count[None, :])


def owner_kernel(part_ref, ends_ref, lists_ref, message_hbm, self_hbm, *refs):
    outs = refs[: 2 * MESSAGES]
    table, stage, pick, rows, acc, raw, aligned, weights, offsets, places, ready, sems, place_sem, out_sems = refs[2 * MESSAGES :]
    items = message_hbm.shape[0]
    width = message_hbm.shape[1]
    tiles = width // LANES
    per_table = items // STAGE
    step = pl.program_id(0)
    devices = pl.num_programs(0)
    part = part_ref[0] * SIDE + part_ref[1]
    negatives = pick.shape[0]
    quarter = negatives // 4

    def asker(i):
        x = (part_ref[0] + i // SIDE) % SIDE
        y = (part_ref[1] + i % SIDE) % SIDE
        return x * SIDE + y

    def range_of(r):
        return jnp.where(part == 0, 0, ends_ref[r, jnp.maximum(part - 1, 0)]), ends_ref[r, part]

    def place_copy():
        return pltpu.make_async_copy(offsets, places, place_sem)

    def place(r, first):
        base = first >> 7
        skip = first & (LANES - 1)
        for c in range(BLOCK + 1):
            raw[c : c + 1, :] = lists_ref[r, pl.ds(base + c, 1), :]
        ahead = lax.broadcasted_iota(jnp.int32, (16, LANES), 1) < LANES - skip
        turn = (LANES - skip) & (LANES - 1)
        aligned[...] = jnp.where(ahead, pltpu.roll(raw[0:16, :], turn, 1), pltpu.roll(raw[1:17, :], turn, 1))
        for half in range(2):
            at = slice(8 * half, 8 * half + 8)
            lines = aligned[at, :]
            offsets[at, :] = (lines & 16383) * tiles
            v = (lines >> 16) & (negatives - 1)
            count = jnp.zeros_like(v)
            for q in range(negatives // LANES):
                counts = jnp.broadcast_to(lists_ref[r, COUNTS + q : COUNTS + q + 1, :], v.shape)
                found = jnp.take_along_axis(counts, v & (LANES - 1), axis=1, mode="promise_in_bounds")
                count = jnp.where(v >> 7 == q, found, count)
            weights[at, :] = jnp.where((lines & 8192) != 0, count, 1).astype(jnp.float32)
        place_copy().start()

    def stage_copy(c):
        source = message_hbm if c < per_table else self_hbm
        return pltpu.make_async_copy(
            source.at[pl.ds((c % per_table) * STAGE, STAGE), :], stage.at[c % DEEP], sems.at[c % DEEP]
        )

    def out_copy(slot, q, array, at):
        return pltpu.make_async_copy(
            ready.at[slot, pl.ds(q * quarter, quarter), :], array.at[at], out_sems.at[slot, q]
        )

    def wait_out(slot):
        for q in range(4):
            out_copy(slot, q, outs[0], 0).wait()

    @pl.when(step == 0)
    def _():
        for c in range(DEEP):
            stage_copy(c).start()
        raw[...] = jnp.zeros_like(raw)
        place(asker(0), range_of(asker(0))[0])
        rows[...] = jnp.zeros_like(rows)
        for c in range(2 * per_table):
            stage_copy(c).wait()

            def spread(i, _, c=c):
                for u in range(4):
                    at = pl.multiple_of(i * 64 + u * 16, 16)
                    block = stage[c % DEEP, pl.ds(at, 16), :].astype(jnp.float32)
                    for half in range(2):
                        for j in range(tiles):
                            first = (c * STAGE + at + half * 8) * tiles + j
                            table[pl.ds(first, 8, stride=tiles), :] = block[
                                half * 8 : half * 8 + 8, j * LANES : (j + 1) * LANES
                            ]
                return 0

            lax.fori_loop(0, STAGE // 64, spread, 0)
            if c + DEEP < 2 * per_table:
                stage_copy(c + DEEP).start()

    a = asker(step)
    start, end = range_of(a)

    def picked(c, left, line, weight):
        v = lax.broadcasted_iota(jnp.int32, (negatives, LANES), 0)
        at = c * LANES + lax.broadcasted_iota(jnp.int32, (1, LANES), 1)
        who = jnp.where(at < left, line >> 16, -1)
        return jnp.where(v == who, weight, 0.0).astype(jnp.bfloat16)

    def gather(left):
        place_copy().wait()
        for c in range(BLOCK):

            @pl.when(c * LANES < left)
            def _(c=c):
                pick[:, c * LANES : (c + 1) * LANES] = picked(c, left, aligned[c : c + 1, :], weights[c : c + 1, :])
                for e in range(CHUNK):
                    at = pl.multiple_of(places[c, e], tiles)
                    rows[c, pl.ds(e, tiles, stride=STRIDE), :] = table[pl.ds(at, tiles), :]

            @pl.when(c * LANES >= left)
            def _(c=c):
                pick[:, c * LANES : (c + 1) * LANES] = jnp.zeros((negatives, LANES), jnp.bfloat16)

    def gather_more(left):
        place_copy().wait()

        def chunk(c, _):
            cols = pl.ds(pl.multiple_of(c * LANES, LANES), LANES)
            one = pl.ds(c, 1)
            pick[:, cols] = picked(c, left, aligned[one, :], weights[one, :])

            def entry(e, _):
                at = pl.multiple_of(places[c, e], tiles)
                rows[c, pl.ds(e, tiles, stride=STRIDE), :] = table[pl.ds(at, tiles), :]
                return 0

            return lax.fori_loop(0, CHUNK, entry, 0)

        lax.fori_loop(0, BLOCK, chunk, 0)

    def summed(low, high):
        gathered = jnp.concatenate(
            [
                jnp.concatenate(
                    [rows[c, j * STRIDE : j * STRIDE + CHUNK, :].astype(jnp.bfloat16) for j in range(tiles)],
                    axis=1,
                )
                for c in range(low, high)
            ],
            axis=0,
        )
        return jnp.dot(
            pick[:, low * LANES : high * LANES], gathered, preferred_element_type=jnp.float32
        )

    many = end - start
    block = BLOCK * LANES
    gather(many)

    def place_next():
        @pl.when(step + 1 < devices)
        def _():
            following = asker(step + 1)
            place(following, range_of(following)[0])

    @pl.when(many <= block)
    def _():
        place_next()

    acc[...] = summed(0, USUAL)

    @pl.when(many > USUAL * LANES)
    def _():
        acc[...] += summed(USUAL, BLOCK)

    @pl.when(many > block)
    def _():
        def more(i, _):
            place(a, start + i * block)
            gather_more(many - i * block)
            acc[...] += summed(0, BLOCK)
            return 0

        lax.fori_loop(1, (many + block - 1) // block, more, 0)
        place_next()

    slot = step % 2

    @pl.when(step >= 2)
    def _():
        wait_out(slot)

    ready[slot] = acc[...].astype(jnp.bfloat16)
    dx = step // SIDE
    dy = step % SIDE
    for d in range(SIDE):

        @pl.when(dx == d)
        def _(d=d):
            for h in range(2):
                out_copy(slot, h, outs[2 * d + h], dy).start()

        @pl.when(dy == d)
        def _(d=d):
            for h in range(2):
                out_copy(slot, 2 + h, outs[MESSAGES + 2 * d + h], dx).start()

    @pl.when(step + 1 == devices)
    def _():
        wait_out(slot)
        wait_out(1 - slot)


def composed_keys(neighbour_slots, self_slot, neighbour_count, fetch_rows):
    negatives, neighbours = neighbour_slots.shape
    folded = negatives // LANES
    return pl.pallas_call(
        compose_kernel,
        out_shape=[
            jax.ShapeDtypeStruct(((neighbours + 1) * folded, LANES), jnp.int32),
            jax.ShapeDtypeStruct((1, LANES), jnp.int32),
        ],
        name="compose",
    )(
        neighbour_slots.T,
        self_slot[None, :],
        neighbour_count[None, :],
        fetch_rows,
    )


def owner_sums(part, ends, lists, message_part, self_part, negatives):
    devices, _, _ = lists.shape
    items, width = message_part.shape
    tiles = width // LANES
    quarter = [jax.ShapeDtypeStruct((SIDE, negatives // 4, width), jnp.bfloat16)]
    return pl.pallas_call(
        owner_kernel,
        grid=(devices,),
        in_specs=[
            pl.BlockSpec(memory_space=pltpu.SMEM),
            pl.BlockSpec(memory_space=pltpu.SMEM),
            pl.BlockSpec(memory_space=pltpu.VMEM),
            pl.BlockSpec(memory_space=pl.ANY),
            pl.BlockSpec(memory_space=pl.ANY),
        ],
        out_specs=[pl.BlockSpec(memory_space=pl.ANY)] * (2 * MESSAGES),
        out_shape=quarter * (2 * MESSAGES),
        scratch_shapes=[
            pltpu.VMEM((2 * items * tiles, LANES), jnp.float32),
            pltpu.VMEM((DEEP, STAGE, width), jnp.bfloat16),
            pltpu.VMEM((negatives, BLOCK * CHUNK), jnp.bfloat16),
            pltpu.VMEM((BLOCK, tiles * STRIDE, LANES), jnp.float32),
            pltpu.VMEM((negatives, width), jnp.float32),
            pltpu.VMEM((24, LANES), jnp.int32),
            pltpu.VMEM((16, LANES), jnp.int32),
            pltpu.VMEM((16, LANES), jnp.float32),
            pltpu.VMEM((16, LANES), jnp.int32),
            pltpu.SMEM((16, LANES), jnp.int32),
            pltpu.VMEM((2, negatives, width), jnp.bfloat16),
            pltpu.SemaphoreType.DMA((DEEP,)),
            pltpu.SemaphoreType.DMA,
            pltpu.SemaphoreType.DMA((2, 4)),
        ],
        compiler_params=pltpu.CompilerParams(
            dimension_semantics=("arbitrary",), vmem_limit_bytes=60 * 2**20
        ),
        name="owner",
    )(part, ends, lists, message_part, self_part)


def moved(x, along, by):
    def place(i):
        x_at, y_at = divmod(i, SIDE)
        if along == "x":
            return (x_at + by) % SIDE * SIDE + y_at
        return x_at * SIDE + (y_at + by) % SIDE

    return lax.ppermute(x, "neg", [(i, place(i)) for i in range(SIDE * SIDE)])


def joined(*parts):
    return sum(p.astype(jnp.float32) for p in parts)


def ring_sums(parts, along):
    far_up = moved(parts[2][0], along, 1)
    far_down = moved(parts[2][1], along, -1)
    near_up = moved(parts[1][1], along, 1)
    near_down = moved(parts[3][0], along, -1)
    sent_up = moved(joined(parts[1][0], far_up).astype(jnp.bfloat16), along, 1)
    sent_down = moved(joined(parts[3][1], far_down).astype(jnp.bfloat16), along, -1)
    return joined(parts[0][0], sent_up, near_down), joined(parts[0][1], near_up, sent_down)


def joint_sums(own_first, own_second, up, down, next_up, next_down, along):
    half = up.shape[0] // 2
    came_up = moved(up, along, 1)
    came_down = moved(down, along, -1)
    sent_up = moved(joined(next_up, came_up[:half]).astype(jnp.bfloat16), along, 1)
    sent_down = moved(joined(next_down, came_down[:half]).astype(jnp.bfloat16), along, -1)
    return joined(own_first, sent_up, came_down[half:]), joined(own_second, came_up[half:], sent_down)


def scattered_sums(outs):
    result = []
    for at, order in ((0, "xy"), (MESSAGES, "yx")):
        parts = [outs[at + 2 * d : at + 2 * d + 2] for d in range(SIDE)]
        first, second = ring_sums(parts, order[0])
        low_first, low_second = first.astype(jnp.bfloat16), second.astype(jnp.bfloat16)
        up = jnp.concatenate([low_first[2:3], low_second[1:2]], axis=0)
        down = jnp.concatenate([low_second[2:3], low_first[3:4]], axis=0)
        result += joint_sums(first[0:1], second[0:1], up, down, low_first[1:2], low_second[3:4], order[1])
    return result


def turned(x, deep, other):
    def place(i):
        z, core = divmod(i, 2)
        return (z + deep) % SIDE * 2 + (1 - core if other else core)

    return lax.ppermute(x, "qry", [(i, place(i)) for i in range(2 * SIDE)])


def all_queries(queries):
    up = turned(queries, 1, False)
    down = turned(queries, -1, False)
    other = turned(queries, 0, True)
    far = turned(up, 1, False)
    other_up = turned(up, 0, True)
    other_down = turned(down, 0, True)
    other_far = turned(far, 0, True)
    return [queries, up, far, down, other, other_up, other_far, other_down]


def table_kernel(items_ref, message_ref, bias_ref, neighbour_ref, self_ref, message_out, self_out):
    f32 = jnp.float32
    items = items_ref[...]
    message = jnp.dot(items, message_ref[...], preferred_element_type=f32) + bias_ref[...]
    message = jnp.maximum(message, 0.0).astype(jnp.bfloat16)
    message_out[...] = jnp.dot(message, neighbour_ref[...], preferred_element_type=f32).astype(jnp.bfloat16)
    self_out[...] = jnp.dot(items, self_ref[...], preferred_element_type=f32).astype(jnp.bfloat16)


def tables(items_table, message_weight, message_bias, neighbour_weight, self_weight):
    items, width = items_table.shape
    weight = pl.BlockSpec((width, width), lambda i: (0, 0))
    block = pl.BlockSpec((STAGE, width), lambda i: (i, 0))
    return pl.pallas_call(
        table_kernel,
        grid=(items // STAGE,),
        in_specs=[block, weight, pl.BlockSpec((1, width), lambda i: (0, 0)), weight, weight],
        out_specs=[block, block],
        out_shape=[jax.ShapeDtypeStruct((items, width), jnp.bfloat16)] * 2,
        compiler_params=pltpu.CompilerParams(dimension_semantics=("arbitrary",)),
        name="tables",
    )(items_table, message_weight, message_bias[None, :], neighbour_weight, self_weight)


def score_kernel(*refs):
    sums = refs[:4]
    count_ref, bias_ref, log_ref, place_ref = refs[4:8]
    queries = refs[8 : 8 + 2 * SIDE]
    embed_ref, lse_ref, held, even, odd, logs, sems = refs[8 + 2 * SIDE :]
    f32 = jnp.float32
    rows = queries[0].shape[0]
    blocks = len(queries) * rows // SCORED
    per_query = rows // SCORED

    def copy(j, source):
        return pltpu.make_async_copy(source, held.at[pl.ds(j * rows, rows), :], sems.at[j])

    for j, source in enumerate(queries):
        copy(j, source).start()
    negatives, width = embed_ref.shape

    def columns(row):
        return jnp.broadcast_to(row, (LANES, negatives)).T

    own = log_ref[pl.ds(place_ref[0], 1), :]
    logs[...] = columns(jnp.log(own.astype(f32)) * LOG2E)
    counts = columns(count_ref[...].astype(f32))
    quarter = negatives // 4
    for q in range(4):
        at = slice(q * quarter, (q + 1) * quarter)
        count = jnp.concatenate([counts[at, :]] * (width // LANES), axis=1)
        hidden = jnp.maximum(sums[q][...] / count + bias_ref[...], 0.0)
        scale_inv = lax.rsqrt(jnp.mean(hidden * hidden, axis=-1, keepdims=True) + 0.25)
        embed_ref[at, :] = (hidden * scale_inv).astype(jnp.bfloat16)

    def products(i):
        block = held[pl.ds(pl.multiple_of(i * SCORED, SCORED), SCORED), :]
        return lax.dot_general(embed_ref[...], block, (((1,), (1,)), ((), ())), preferred_element_type=f32)

    def reduced(ref, i):
        found = []
        for j in range(SCORED // LANES):
            lane = slice(j * LANES, (j + 1) * LANES)
            scores = ref[:, lane] * (0.25 * LOG2E) - logs[...]
            peak = jnp.max(scores, axis=0, keepdims=True)
            total = jnp.sum(jnp.exp2(scores - peak), axis=0, keepdims=True)
            found.append((peak + jnp.log2(total)) * (1.0 / LOG2E))
        lse_ref[pl.ds(i, 1), :] = jnp.concatenate(found, axis=1)

    copy(0, queries[0]).wait()
    even[...] = products(0)

    def pair(i, _):
        following = jnp.minimum(2 * i + 2, blocks - 1)

        @pl.when((following % per_query == 0) & (2 * i + 2 < blocks))
        def _():
            copy(following // per_query, queries[0]).wait()

        odd[...] = products(2 * i + 1)
        reduced(even, 2 * i)
        even[...] = products(following)
        reduced(odd, 2 * i + 1)
        return 0

    lax.fori_loop(0, blocks // 2, pair, 0)


def scored(sums, count, bias, counts_all, place, queries):
    negatives = count.shape[0]
    rows, width = queries[0].shape
    total = rows * len(queries)
    in_vmem = pl.BlockSpec(memory_space=pltpu.VMEM)
    return pl.pallas_call(
        score_kernel,
        in_specs=[in_vmem] * 7
        + [pl.BlockSpec(memory_space=pltpu.SMEM)]
        + [pl.BlockSpec(memory_space=pl.ANY)] * len(queries),
        out_specs=[in_vmem] * 2,
        out_shape=[
            jax.ShapeDtypeStruct((negatives, width), jnp.bfloat16),
            jax.ShapeDtypeStruct((total // SCORED, SCORED), jnp.float32),
        ],
        scratch_shapes=[
            pltpu.VMEM((total, width), jnp.bfloat16),
            pltpu.VMEM((negatives, SCORED), jnp.float32),
            pltpu.VMEM((negatives, SCORED), jnp.float32),
            pltpu.VMEM((negatives, LANES), jnp.float32),
            pltpu.SemaphoreType.DMA((len(queries),)),
        ],
        name="score",
    )(*sums, count[None, :], bias[None, :], counts_all, place, *queries)


def per_device(
    items_table,
    fetch_rows,
    neighbour_slots,
    neighbour_count,
    self_slot,
    negative_count,
    message_weight,
    message_bias,
    self_weight,
    neighbour_weight,
    output_bias,
    queries,
):
    negatives = neighbour_count.shape[0]
    parts = lax.axis_size("neg")
    groups = lax.axis_size("qry")
    query_blocks = all_queries(queries)

    keys, ends = composed_keys(neighbour_slots, self_slot, neighbour_count, fetch_rows)
    ordered = lax.sort(keys.reshape(-1), is_stable=False).reshape(keys.shape)
    lists = packed_lists(ordered, ends, neighbour_count, parts)
    lists = lax.all_to_all(lists, "neg", split_axis=0, concat_axis=0, tiled=True)

    message_part, self_part = tables(items_table, message_weight, message_bias, neighbour_weight, self_weight)

    place = lax.axis_index("neg")
    part = jnp.stack([place // SIDE, place % SIDE]).astype(jnp.int32)
    outs = owner_sums(part, lists[:, keys.shape[0], :parts], lists, message_part, self_part, negatives)
    sums = [q[0] for q in scattered_sums(outs)]

    here = lax.axis_index("qry")
    counts_all = negative_count.reshape(groups, negatives)
    negative_embed, part_lse = scored(
        sums, neighbour_count, output_bias, counts_all, here.reshape(1), query_blocks
    )
    z, core = here // 2, here % 2
    group = jnp.arange(groups)
    source = ((z - group // 2) % SIDE) + SIDE * ((group % 2) ^ core)
    picked = source[:, None] == group[None, :]
    blocks = part_lse.reshape(groups, -1)
    blocks = jnp.sum(jnp.where(picked[:, :, None], blocks[None], 0.0), axis=1)
    shared = jnp.broadcast_to(blocks[None], (parts, groups, queries.shape[0]))
    parts_lse = lax.all_to_all(
        shared.reshape(parts * groups, -1), ("neg", "qry"), split_axis=0, concat_axis=0, tiled=True
    )
    top = jnp.max(parts_lse, axis=0)
    query_lse = top + jnp.log(jnp.sum(jnp.exp(parts_lse - top[None, :]), axis=0))
    return (negative_embed, query_lse - math.log(negatives * parts * groups))


def solution(mesh):
    in_specs = (
        P("neg", None),
        P(("neg", "qry"), None),
        P(("neg", "qry"), None),
        P(("neg", "qry")),
        P(("neg", "qry")),
        P("neg"),
        P(),
        P(),
        P(),
        P(),
        P(),
        P("qry", None),
    )
    out_specs = (P(("neg", "qry"), None), P("qry"))

    return jax.shard_map(per_device, mesh=mesh, in_specs=in_specs, out_specs=out_specs, check_vma=False)
```

```python
import math

import jax
import jax.numpy as jnp
from jax import lax
from jax.experimental import pallas as pl
from jax.experimental.pallas import tpu as pltpu
from jax.sharding import PartitionSpec as P


LANES = 128
DEAD = 2**31 - 1
CHUNK = 128
STRIDE = 132
BLOCK = 10
USUAL = 8
STAGE = 1024
DEEP = 8
LINES = 176
COUNTS = 165
SIDE = 4
SCORED = 1024
LOG2E = 1.4426950408889634
MESSAGES = 2 * SIDE


def compose_kernel(slots_ref, self_ref, count_ref, fetch_ref, keys_ref, ends_ref):
    neighbours, negatives = slots_ref.shape
    parts, per_part = fetch_ref.shape
    per_line = per_part // LANES
    half = parts // 2
    packed = fetch_ref[:half, :] | (fetch_ref[half:, :] << 13)
    lines = [
        jnp.broadcast_to(packed[p : p + 1, j * LANES : (j + 1) * LANES], (8, LANES))
        for p in range(half)
        for j in range(per_line)
    ]

    def located(slot):
        hi = slot >> 7
        lo = slot & 127
        upper = hi >= len(lines)
        folded = jnp.where(upper, hi - len(lines), hi)
        found = jnp.zeros_like(slot)
        for h, line in enumerate(lines):
            at = jnp.take_along_axis(line, lo, axis=1, mode="promise_in_bounds")
            found = jnp.where(folded == h, at, found)
        row = jnp.where(upper, found >> 13, found & 8191)
        return ((((hi * 205) >> 10) - 8) << 28) | row

    sublane = lax.broadcasted_iota(jnp.int32, (8, LANES), 0)
    lane = lax.broadcasted_iota(jnp.int32, (8, LANES), 1)
    for j in range(negatives // LANES):
        cols = slice(j * LANES, (j + 1) * LANES)
        count = jnp.broadcast_to(count_ref[:, cols], (8, LANES))
        for i in range(neighbours // 8):
            key = located(slots_ref[8 * i : 8 * (i + 1), cols]) | ((lane + j * LANES) << 19)
            first = (j * (neighbours // 8) + i) * 8
            keys_ref[first : first + 8, :] = jnp.where(sublane + 8 * i < count, key, DEAD)

    def tile_of(ref):
        tiles = [ref[:, j * LANES : (j + 1) * LANES] for j in range(negatives // LANES)]
        return jnp.concatenate(tiles + [jnp.zeros((8 - len(tiles), LANES), jnp.int32)], axis=0)

    own = located(tile_of(self_ref)) | ((sublane * LANES + lane) << 19)
    own = own | ((tile_of(count_ref) - 20) << 14) | (1 << 13)
    keys_ref[neighbours * negatives // LANES :, :] = own[: negatives // LANES]

    keys = keys_ref[...]
    at = lax.broadcasted_iota(jnp.int32, (1, LANES), 1)
    ends = jnp.zeros((1, LANES), jnp.int32)
    for p in range(parts):
        below = jnp.sum((keys < min((p + 1 - 8) << 28, DEAD)).astype(jnp.int32), axis=0, keepdims=True)
        ends = jnp.where(at == p, jnp.sum(below, axis=1, keepdims=True), ends)
    ends_ref[...] = ends


def pack_kernel(keys_ref, ends_ref, count_ref, out_ref):
    entries = keys_ref.shape[0]
    negatives = count_ref.shape[1]
    keys = keys_ref[...]
    lines = (((keys >> 19) & (negatives - 1)) << 16) | (keys & 16383)
    count = [count_ref[:, q * LANES : (q + 1) * LANES] for q in range(negatives // LANES)]
    for p in range(out_ref.shape[0]):
        out_ref[p, :entries, :] = lines
        out_ref[p, entries : entries + 1, :] = ends_ref[...]
        for q, line in enumerate(count):
            out_ref[p, COUNTS + q : COUNTS + q + 1, :] = line
        out_ref[p, COUNTS + len(count) :, :] = jnp.zeros((LINES - COUNTS - len(count), LANES), jnp.int32)


def packed_lists(keys, ends, neighbour_count, devices):
    return pl.pallas_call(
        pack_kernel,
        out_shape=jax.ShapeDtypeStruct((devices, LINES, LANES), jnp.int32),
        name="pack",
    )(keys, ends, neighbour_count[None, :])


def owner_kernel(part_ref, ends_ref, lists_ref, message_hbm, self_hbm, *refs):
    outs = refs[: 2 * MESSAGES]
    table, stage, pick, rows, acc, raw, aligned, weights, offsets, places, ready, sems, place_sem, out_sems = refs[2 * MESSAGES :]
    items = message_hbm.shape[0]
    width = message_hbm.shape[1]
    tiles = width // LANES
    per_table = items // STAGE
    step = pl.program_id(0)
    devices = pl.num_programs(0)
    part = part_ref[0] * SIDE + part_ref[1]
    negatives = pick.shape[0]
    quarter = negatives // 4

    def asker(i):
        x = (part_ref[0] + i // SIDE) % SIDE
        y = (part_ref[1] + i % SIDE) % SIDE
        return x * SIDE + y

    def range_of(r):
        return jnp.where(part == 0, 0, ends_ref[r, jnp.maximum(part - 1, 0)]), ends_ref[r, part]

    def place_copy():
        return pltpu.make_async_copy(offsets, places, place_sem)

    def place(r, first):
        base = first >> 7
        skip = first & (LANES - 1)
        for c in range(BLOCK + 1):
            raw[c : c + 1, :] = lists_ref[r, pl.ds(base + c, 1), :]
        ahead = lax.broadcasted_iota(jnp.int32, (16, LANES), 1) < LANES - skip
        turn = (LANES - skip) & (LANES - 1)
        aligned[...] = jnp.where(ahead, pltpu.roll(raw[0:16, :], turn, 1), pltpu.roll(raw[1:17, :], turn, 1))
        for half in range(2):
            at = slice(8 * half, 8 * half + 8)
            lines = aligned[at, :]
            offsets[at, :] = (lines & 16383) * tiles
            v = (lines >> 16) & (negatives - 1)
            count = jnp.zeros_like(v)
            for q in range(negatives // LANES):
                counts = jnp.broadcast_to(lists_ref[r, COUNTS + q : COUNTS + q + 1, :], v.shape)
                found = jnp.take_along_axis(counts, v & (LANES - 1), axis=1, mode="promise_in_bounds")
                count = jnp.where(v >> 7 == q, found, count)
            weights[at, :] = jnp.where((lines & 8192) != 0, count, 1).astype(jnp.float32)
        place_copy().start()

    def stage_copy(c):
        source = message_hbm if c < per_table else self_hbm
        return pltpu.make_async_copy(
            source.at[pl.ds((c % per_table) * STAGE, STAGE), :], stage.at[c % DEEP], sems.at[c % DEEP]
        )

    def out_copy(slot, q, array, at):
        return pltpu.make_async_copy(
            ready.at[slot, pl.ds(q * quarter, quarter), :], array.at[at], out_sems.at[slot, q]
        )

    def wait_out(slot):
        for q in range(4):
            out_copy(slot, q, outs[0], 0).wait()

    @pl.when(step == 0)
    def _():
        for c in range(DEEP):
            stage_copy(c).start()
        raw[...] = jnp.zeros_like(raw)
        place(asker(0), range_of(asker(0))[0])
        rows[...] = jnp.zeros_like(rows)
        for c in range(2 * per_table):
            stage_copy(c).wait()

            def spread(i, _, c=c):
                for u in range(4):
                    at = pl.multiple_of(i * 64 + u * 16, 16)
                    block = stage[c % DEEP, pl.ds(at, 16), :].astype(jnp.float32)
                    for half in range(2):
                        for j in range(tiles):
                            first = (c * STAGE + at + half * 8) * tiles + j
                            table[pl.ds(first, 8, stride=tiles), :] = block[
                                half * 8 : half * 8 + 8, j * LANES : (j + 1) * LANES
                            ]
                return 0

            lax.fori_loop(0, STAGE // 64, spread, 0)
            if c + DEEP < 2 * per_table:
                stage_copy(c + DEEP).start()

    a = asker(step)
    start, end = range_of(a)

    def picked(c, left, line, weight):
        v = lax.broadcasted_iota(jnp.int32, (negatives, LANES), 0)
        at = c * LANES + lax.broadcasted_iota(jnp.int32, (1, LANES), 1)
        who = jnp.where(at < left, line >> 16, -1)
        return jnp.where(v == who, weight, 0.0).astype(jnp.bfloat16)

    def gather(left):
        place_copy().wait()
        for c in range(BLOCK):

            @pl.when(c * LANES < left)
            def _(c=c):
                pick[:, c * LANES : (c + 1) * LANES] = picked(c, left, aligned[c : c + 1, :], weights[c : c + 1, :])
                for e in range(CHUNK):
                    at = pl.multiple_of(places[c, e], tiles)
                    rows[c, pl.ds(e, tiles, stride=STRIDE), :] = table[pl.ds(at, tiles), :]

            @pl.when(c * LANES >= left)
            def _(c=c):
                pick[:, c * LANES : (c + 1) * LANES] = jnp.zeros((negatives, LANES), jnp.bfloat16)

    def gather_more(left):
        place_copy().wait()

        def chunk(c, _):
            cols = pl.ds(pl.multiple_of(c * LANES, LANES), LANES)
            one = pl.ds(c, 1)
            pick[:, cols] = picked(c, left, aligned[one, :], weights[one, :])

            def entry(e, _):
                at = pl.multiple_of(places[c, e], tiles)
                rows[c, pl.ds(e, tiles, stride=STRIDE), :] = table[pl.ds(at, tiles), :]
                return 0

            return lax.fori_loop(0, CHUNK, entry, 0)

        lax.fori_loop(0, BLOCK, chunk, 0)

    def summed(low, high):
        gathered = jnp.concatenate(
            [
                jnp.concatenate(
                    [rows[c, j * STRIDE : j * STRIDE + CHUNK, :].astype(jnp.bfloat16) for j in range(tiles)],
                    axis=1,
                )
                for c in range(low, high)
            ],
            axis=0,
        )
        return jnp.dot(
            pick[:, low * LANES : high * LANES], gathered, preferred_element_type=jnp.float32
        )

    many = end - start
    block = BLOCK * LANES
    gather(many)

    def place_next():
        @pl.when(step + 1 < devices)
        def _():
            following = asker(step + 1)
            place(following, range_of(following)[0])

    @pl.when(many <= block)
    def _():
        place_next()

    acc[...] = summed(0, USUAL)

    @pl.when(many > USUAL * LANES)
    def _():
        acc[...] += summed(USUAL, BLOCK)

    @pl.when(many > block)
    def _():
        def more(i, _):
            place(a, start + i * block)
            gather_more(many - i * block)
            acc[...] += summed(0, BLOCK)
            return 0

        lax.fori_loop(1, (many + block - 1) // block, more, 0)
        place_next()

    slot = step % 2

    @pl.when(step >= 2)
    def _():
        wait_out(slot)

    ready[slot] = acc[...].astype(jnp.bfloat16)
    dx = step // SIDE
    dy = step % SIDE
    for d in range(SIDE):

        @pl.when(dx == d)
        def _(d=d):
            for h in range(2):
                out_copy(slot, h, outs[2 * d + h], dy).start()

        @pl.when(dy == d)
        def _(d=d):
            for h in range(2):
                out_copy(slot, 2 + h, outs[MESSAGES + 2 * d + h], dx).start()

    @pl.when(step + 1 == devices)
    def _():
        wait_out(slot)
        wait_out(1 - slot)


def composed_keys(neighbour_slots, self_slot, neighbour_count, fetch_rows):
    negatives, neighbours = neighbour_slots.shape
    folded = negatives // LANES
    return pl.pallas_call(
        compose_kernel,
        out_shape=[
            jax.ShapeDtypeStruct(((neighbours + 1) * folded, LANES), jnp.int32),
            jax.ShapeDtypeStruct((1, LANES), jnp.int32),
        ],
        name="compose",
    )(
        neighbour_slots.T,
        self_slot[None, :],
        neighbour_count[None, :],
        fetch_rows,
    )


def owner_sums(part, ends, lists, message_part, self_part, negatives):
    devices, _, _ = lists.shape
    items, width = message_part.shape
    tiles = width // LANES
    quarter = [jax.ShapeDtypeStruct((SIDE, negatives // 4, width), jnp.bfloat16)]
    return pl.pallas_call(
        owner_kernel,
        grid=(devices,),
        in_specs=[
            pl.BlockSpec(memory_space=pltpu.SMEM),
            pl.BlockSpec(memory_space=pltpu.SMEM),
            pl.BlockSpec(memory_space=pltpu.VMEM),
            pl.BlockSpec(memory_space=pl.ANY),
            pl.BlockSpec(memory_space=pl.ANY),
        ],
        out_specs=[pl.BlockSpec(memory_space=pl.ANY)] * (2 * MESSAGES),
        out_shape=quarter * (2 * MESSAGES),
        scratch_shapes=[
            pltpu.VMEM((2 * items * tiles, LANES), jnp.float32),
            pltpu.VMEM((DEEP, STAGE, width), jnp.bfloat16),
            pltpu.VMEM((negatives, BLOCK * CHUNK), jnp.bfloat16),
            pltpu.VMEM((BLOCK, tiles * STRIDE, LANES), jnp.float32),
            pltpu.VMEM((negatives, width), jnp.float32),
            pltpu.VMEM((24, LANES), jnp.int32),
            pltpu.VMEM((16, LANES), jnp.int32),
            pltpu.VMEM((16, LANES), jnp.float32),
            pltpu.VMEM((16, LANES), jnp.int32),
            pltpu.SMEM((16, LANES), jnp.int32),
            pltpu.VMEM((2, negatives, width), jnp.bfloat16),
            pltpu.SemaphoreType.DMA((DEEP,)),
            pltpu.SemaphoreType.DMA,
            pltpu.SemaphoreType.DMA((2, 4)),
        ],
        compiler_params=pltpu.CompilerParams(
            dimension_semantics=("arbitrary",), vmem_limit_bytes=60 * 2**20
        ),
        name="owner",
    )(part, ends, lists, message_part, self_part)


def moved(x, along, by):
    def place(i):
        x_at, y_at = divmod(i, SIDE)
        if along == "x":
            return (x_at + by) % SIDE * SIDE + y_at
        return x_at * SIDE + (y_at + by) % SIDE

    return lax.ppermute(x, "neg", [(i, place(i)) for i in range(SIDE * SIDE)])


def joined(*parts):
    return sum(p.astype(jnp.float32) for p in parts)


def ring_sums(parts, along):
    far_up = moved(parts[2][0], along, 1)
    far_down = moved(parts[2][1], along, -1)
    near_up = moved(parts[1][1], along, 1)
    near_down = moved(parts[3][0], along, -1)
    sent_up = moved(joined(parts[1][0], far_up).astype(jnp.bfloat16), along, 1)
    sent_down = moved(joined(parts[3][1], far_down).astype(jnp.bfloat16), along, -1)
    return joined(parts[0][0], sent_up, near_down), joined(parts[0][1], near_up, sent_down)


def joint_sums(own_first, own_second, up, down, next_up, next_down, along):
    half = up.shape[0] // 2
    came_up = moved(up, along, 1)
    came_down = moved(down, along, -1)
    sent_up = moved(joined(next_up, came_up[:half]).astype(jnp.bfloat16), along, 1)
    sent_down = moved(joined(next_down, came_down[:half]).astype(jnp.bfloat16), along, -1)
    return joined(own_first, sent_up, came_down[half:]), joined(own_second, came_up[half:], sent_down)


def scattered_sums(outs):
    result = []
    for at, order in ((0, "xy"), (MESSAGES, "yx")):
        parts = [outs[at + 2 * d : at + 2 * d + 2] for d in range(SIDE)]
        first, second = ring_sums(parts, order[0])
        low_first, low_second = first.astype(jnp.bfloat16), second.astype(jnp.bfloat16)
        up = jnp.concatenate([low_first[2:3], low_second[1:2]], axis=0)
        down = jnp.concatenate([low_second[2:3], low_first[3:4]], axis=0)
        result += joint_sums(first[0:1], second[0:1], up, down, low_first[1:2], low_second[3:4], order[1])
    return result


def turned(x, deep, other):
    def place(i):
        z, core = divmod(i, 2)
        return (z + deep) % SIDE * 2 + (1 - core if other else core)

    return lax.ppermute(x, "qry", [(i, place(i)) for i in range(2 * SIDE)])


def all_queries(queries):
    up = turned(queries, 1, False)
    down = turned(queries, -1, False)
    other = turned(queries, 0, True)
    far = turned(up, 1, False)
    other_up = turned(up, 0, True)
    other_down = turned(down, 0, True)
    other_far = turned(far, 0, True)
    return [queries, up, far, down, other, other_up, other_far, other_down]


def table_kernel(items_ref, message_ref, bias_ref, neighbour_ref, self_ref, message_out, self_out):
    f32 = jnp.float32
    items = items_ref[...]
    message = jnp.dot(items, message_ref[...], preferred_element_type=f32) + bias_ref[...]
    message = jnp.maximum(message, 0.0).astype(jnp.bfloat16)
    message_out[...] = jnp.dot(message, neighbour_ref[...], preferred_element_type=f32).astype(jnp.bfloat16)
    self_out[...] = jnp.dot(items, self_ref[...], preferred_element_type=f32).astype(jnp.bfloat16)


def tables(items_table, message_weight, message_bias, neighbour_weight, self_weight):
    items, width = items_table.shape
    weight = pl.BlockSpec((width, width), lambda i: (0, 0))
    block = pl.BlockSpec((STAGE, width), lambda i: (i, 0))
    return pl.pallas_call(
        table_kernel,
        grid=(items // STAGE,),
        in_specs=[block, weight, pl.BlockSpec((1, width), lambda i: (0, 0)), weight, weight],
        out_specs=[block, block],
        out_shape=[jax.ShapeDtypeStruct((items, width), jnp.bfloat16)] * 2,
        compiler_params=pltpu.CompilerParams(dimension_semantics=("arbitrary",)),
        name="tables",
    )(items_table, message_weight, message_bias[None, :], neighbour_weight, self_weight)


def score_kernel(*refs):
    sums = refs[:4]
    count_ref, bias_ref, log_ref, place_ref = refs[4:8]
    queries = refs[8 : 8 + 2 * SIDE]
    embed_ref, lse_ref, held, even, odd, logs, sems = refs[8 + 2 * SIDE :]
    f32 = jnp.float32
    rows = queries[0].shape[0]
    blocks = len(queries) * rows // SCORED
    per_query = rows // SCORED

    def copy(j, source):
        return pltpu.make_async_copy(source, held.at[pl.ds(j * rows, rows), :], sems.at[j])

    for j, source in enumerate(queries):
        copy(j, source).start()
    negatives, width = embed_ref.shape

    def columns(row):
        return jnp.broadcast_to(row, (LANES, negatives)).T

    own = log_ref[:, pl.ds(pl.multiple_of(place_ref[0] * negatives, negatives), negatives)]
    logs[...] = columns(jnp.log(own.astype(f32)) * LOG2E)
    counts = columns(count_ref[...].astype(f32))
    quarter = negatives // 4
    for q in range(4):
        at = slice(q * quarter, (q + 1) * quarter)
        count = jnp.concatenate([counts[at, :]] * (width // LANES), axis=1)
        hidden = jnp.maximum(sums[q][...] / count + bias_ref[...], 0.0)
        scale_inv = lax.rsqrt(jnp.mean(hidden * hidden, axis=-1, keepdims=True) + 0.25)
        embed_ref[at, :] = (hidden * scale_inv).astype(jnp.bfloat16)

    def products(i):
        block = held[pl.ds(pl.multiple_of(i * SCORED, SCORED), SCORED), :]
        return lax.dot_general(embed_ref[...], block, (((1,), (1,)), ((), ())), preferred_element_type=f32)

    def reduced(ref, i):
        found = []
        for j in range(SCORED // LANES):
            lane = slice(j * LANES, (j + 1) * LANES)
            scores = ref[:, lane] * (0.25 * LOG2E) - logs[...]
            peak = jnp.max(scores, axis=0, keepdims=True)
            total = jnp.sum(jnp.exp2(scores - peak), axis=0, keepdims=True)
            found.append((peak + jnp.log2(total)) * (1.0 / LOG2E))
        found = jnp.concatenate(found, axis=1)
        z, core = place_ref[0] >> 1, place_ref[0] & 1
        group = ((z - (i & (SIDE - 1))) & (SIDE - 1)) * 2 + (core ^ (i // SIDE))
        for a in range(lse_ref.shape[0] // len(queries)):
            lse_ref[a * len(queries) + group] = found

    copy(0, queries[0]).wait()
    even[...] = products(0)

    def pair(i, _):
        following = jnp.minimum(2 * i + 2, blocks - 1)
        if per_query == 1:
            copy(2 * i + 1, queries[0]).wait()

        @pl.when((following % per_query == 0) & (2 * i + 2 < blocks))
        def _():
            copy(following // per_query, queries[0]).wait()

        odd[...] = products(2 * i + 1)
        reduced(even, 2 * i)
        even[...] = products(following)
        reduced(odd, 2 * i + 1)
        return 0

    lax.fori_loop(0, blocks // 2, pair, 0)


def scored(sums, count, bias, counts_all, place, queries, parts):
    negatives = count.shape[0]
    rows, width = queries[0].shape
    total = rows * len(queries)
    in_vmem = pl.BlockSpec(memory_space=pltpu.VMEM)
    return pl.pallas_call(
        score_kernel,
        in_specs=[in_vmem] * 7
        + [pl.BlockSpec(memory_space=pltpu.SMEM)]
        + [pl.BlockSpec(memory_space=pl.ANY)] * len(queries),
        out_specs=[in_vmem] * 2,
        out_shape=[
            jax.ShapeDtypeStruct((negatives, width), jnp.bfloat16),
            jax.ShapeDtypeStruct((parts * len(queries), 1, rows), jnp.float32),
        ],
        scratch_shapes=[
            pltpu.VMEM((total, width), jnp.bfloat16),
            pltpu.VMEM((negatives, SCORED), jnp.float32),
            pltpu.VMEM((negatives, SCORED), jnp.float32),
            pltpu.VMEM((negatives, LANES), jnp.float32),
            pltpu.SemaphoreType.DMA((len(queries),)),
        ],
        name="score",
    )(*sums, count[None, :], bias[None, :], counts_all, place, *queries)


def per_device(
    items_table,
    fetch_rows,
    neighbour_slots,
    neighbour_count,
    self_slot,
    negative_count,
    message_weight,
    message_bias,
    self_weight,
    neighbour_weight,
    output_bias,
    queries,
):
    negatives = neighbour_count.shape[0]
    parts = lax.axis_size("neg")
    groups = lax.axis_size("qry")
    query_blocks = all_queries(queries)

    keys, ends = composed_keys(neighbour_slots, self_slot, neighbour_count, fetch_rows)
    ordered = lax.sort(keys.reshape(-1), is_stable=False).reshape(keys.shape)
    lists = packed_lists(ordered, ends, neighbour_count, parts)
    lists = lax.all_to_all(lists, "neg", split_axis=0, concat_axis=0, tiled=True)

    message_part, self_part = tables(items_table, message_weight, message_bias, neighbour_weight, self_weight)

    place = lax.axis_index("neg")
    part = jnp.stack([place // SIDE, place % SIDE]).astype(jnp.int32)
    outs = owner_sums(part, lists[:, keys.shape[0], :parts], lists, message_part, self_part, negatives)
    sums = [q[0] for q in scattered_sums(outs)]

    here = lax.axis_index("qry")
    negative_embed, shared = scored(
        sums, neighbour_count, output_bias, negative_count[None, :], here.reshape(1), query_blocks, parts
    )
    parts_lse = lax.all_to_all(shared, ("neg", "qry"), split_axis=0, concat_axis=0, tiled=True)
    parts_lse = parts_lse.reshape(parts * groups, -1)
    top = jnp.max(parts_lse, axis=0)
    query_lse = top + jnp.log(jnp.sum(jnp.exp(parts_lse - top[None, :]), axis=0))
    return (negative_embed, query_lse - math.log(negatives * parts * groups))


def solution(mesh):
    in_specs = (
        P("neg", None),
        P(("neg", "qry"), None),
        P(("neg", "qry"), None),
        P(("neg", "qry")),
        P(("neg", "qry")),
        P("neg"),
        P(),
        P(),
        P(),
        P(),
        P(),
        P("qry", None),
    )
    out_specs = (P(("neg", "qry"), None), P("qry"))

    return jax.shard_map(per_device, mesh=mesh, in_specs=in_specs, out_specs=out_specs, check_vma=False)
```
